512 devices in a mesh: group: 32 (over x, y, core), tp: 16 (over z).
Axes of the slice: x: 4, y: 4, z: 16, core: 2. Of those that a mesh axis runs over, the one named last changes fastest.
Arguments:
- hidden: bfloat16 [8192, 8192], P('group', 'tp'), may hold values from -6 to 6
- w_kv: bfloat16 [8192, 2048], P('tp'), may hold values from -0.0625 to 0.0625
- prompt_lengths: int32 [8, 16], replicated, may hold values from 1 to 128, 256 in all within a row
- owner_step: int32 [8, 16], replicated, may hold values from 1 to 3
- cache: bfloat16 [1024, 128, 2048], P(('group', 'tp')), may hold values from -8 to 8
- cache_len: int32 [1024], P(('group', 'tp')), may hold values from 1 to 128
- queries: bfloat16 [1024, 8192], P('group', 'tp'), may hold values from -200 to 200
- fresh: bfloat16 [1024, 2048], P('group', 'tp'), may hold values from -10 to 10
- logits: bfloat16 [1024, 122880], P('group', 'tp'), may hold values from -300 to 300
- states: int32 [1024], P('group'), may hold values from 0 to 23
- masks: int32 [24, 4096], P(None, 'tp'), may hold values from 0 to 1073741823, as said below
Outputs:
- attended: bfloat16 [1024, 8192], P('group', 'tp')
- logprob: float32 [1024, 122880], P('group', 'tp')
The draws below stay inside these ranges and needn't reach their ends.
Inputs may be any that keep to these rules, and one draw needn't show every extreme that they name: `prompt_lengths`: each row sums to 256; the longest prompt of every row has exactly 128 tokens. Prompt k of prefill group p goes to group p + owner_step[p, k] * 8. `masks`: every state allows at least one token in each aligned block of 7680 vocabulary entries.
All inputs are finite; a program needn't handle non-finite values.
Results may differ from the reference program's by a relative error of at most 0.02.
Values may be sent and summed in bfloat16 or wider, within the bound.
No kernel may reach another device: no remote copies, remote signals or barrier semaphores. Data moves between devices by JAX's collectives and lax.ppermute only.
A program may use at most 64 MiB of HBM per device.

```python
import math
import jax
import jax.numpy as jnp
import numpy as np
from jax import lax

D = 8192
HEADS = 64
KVH = 8
HD = 128
VOC_DEV = 7680
BLOCK = 256
MAXLEN = 128
CACHE = 128
STATES = 24
REQ_DEV = 2
REQUESTS = 32
PROMPTS = 16
VOCAB = 122880
PREFILL = 8
N_GROUP = 32
N_TP = 16


def anchor_draw(key):
    base = jax.random.fold_in(key, 901)
    chosen_rows = jax.random.permutation(jax.random.fold_in(base, 1), PREFILL * REQUESTS)[:6]
    anchors = jnp.clip(jax.random.normal(jax.random.fold_in(base, 2), (6, KVH * HD), jnp.float32), -4.0, 4.0)
    return (chosen_rows, anchors)


def draw_cache(key, part):
    shape = (N_GROUP * REQUESTS, CACHE, 2 * KVH * HD)
    values = jnp.clip(jax.random.normal(jax.random.fold_in(key, 11), shape, jnp.float32), -6.0, 6.0)
    chosen_rows, anchors = anchor_draw(key)
    values = values.at[chosen_rows, 0, :KVH * HD].set(anchors)
    return values.astype(jnp.bfloat16)


def draw_queries(key, part):
    shape = (N_GROUP * REQUESTS, HEADS * HD)
    values = jnp.clip(jax.random.normal(jax.random.fold_in(key, 21), shape, jnp.float32), -6.0, 6.0)
    return values.astype(jnp.bfloat16)


def draw_fresh(key, part):
    shape = (N_GROUP * REQUESTS, 2 * KVH * HD)
    values = jnp.clip(jax.random.normal(jax.random.fold_in(key, 31), shape, jnp.float32), -6.0, 6.0)
    return values.astype(jnp.bfloat16)


def draw_logits(key, part):
    shape = (N_GROUP * REQUESTS, VOCAB)
    ramp = 1.5 * jnp.arange(VOCAB, dtype=jnp.float32) / VOCAB
    values = 3.0 * jnp.clip(jax.random.normal(jax.random.fold_in(key, 41), shape, jnp.float32), -8.0, 8.0) + ramp[None, :]
    return values.astype(jnp.bfloat16)


def draw_masks(key, part):
    word_count = VOCAB // 30
    packed = jax.random.randint(jax.random.fold_in(key, 51), (STATES, word_count), 0, 1073741824, jnp.int32)
    forced = jnp.left_shift(jnp.ones((STATES, word_count), jnp.int32), jax.random.randint(jax.random.fold_in(key, 52), (STATES, word_count), 0, 30, jnp.int32))
    leading = jnp.arange(word_count, dtype=jnp.int32) % (VOC_DEV // 30) == 0
    return jnp.where(leading[None, :], jnp.bitwise_or(packed, forced), packed).astype(jnp.int32)


def touch_ends(values, rng, low, largest):
    extent = values.shape
    spot = [jax.random.randint(jax.random.fold_in(rng, axis), (), 0, extent[axis]) for axis in range(len(extent))]
    values = values.at[tuple(spot)].set(low)
    longest = extent.index(max(extent))
    spot[longest] = (spot[longest] + 1) % extent[longest]
    return values.at[tuple(spot)].set(largest)


def shard_levels(rng, shape, cuts, low, high):
    def one(dim, blocks):
        steps = jax.random.uniform(jax.random.fold_in(jax.random.fold_in(rng, 6), dim), (blocks,), jnp.float32, low / len(cuts), high / len(cuts))
        return jnp.repeat(jnp.exp(steps), shape[dim] // blocks).reshape((-1,) + (1,) * (len(shape) - dim - 1))

    factor_of = one(*cuts[0])
    for cut in cuts[1:]:
        factor_of = factor_of * one(*cut)
    return factor_of


def profile(count, total, limit, slope):
    weights = [(1 << 20) // math.isqrt(rank ** slope) + 1 for rank in range(2, count + 1)]
    surplus, holding = total - limit - (count - 1), [1] * (count - 1)
    while surplus > 0:
        movable = [i for i in range(count - 1) if holding[i] < limit]
        whole, remaining = sum([weights[i] for i in movable]), surplus
        for i in movable:
            extra = min(limit - holding[i], max(1, remaining * weights[i] // whole), surplus)
            holding[i] = holding[i] + extra
            surplus = surplus - extra
    return np.array([limit] + holding)


def uneven_parts(key, count, total, limit, slope):
    if count == 2:
        one = jax.random.randint(key, (), max(1, total - limit), min(limit, total - 1) + 1)
        return jnp.stack([one, total - one])
    tallies = jnp.asarray(profile(count, total, limit, slope), jnp.int32)
    twos = (count - 1) // 2
    giver, sink = tallies[1:1 + 2 * twos:2], tallies[2:2 + 2 * twos:2]
    slack = jnp.minimum(giver - 1, limit - sink)
    moved = jax.random.randint(jax.random.fold_in(key, 1), (twos,), 0, 1 << 20) % (slack + 1)
    tallies = tallies.at[1:1 + 2 * twos:2].set(giver - moved).at[2:2 + 2 * twos:2].set(sink + moved)
    return tallies[jax.random.permutation(jax.random.fold_in(key, 2), count)]


def normal_values(key, dims, scale, bound, pieces=(), kind=jnp.bfloat16):
    entries = jax.random.normal(key, dims, jnp.float32) * scale
    if len(pieces) > 0:
        entries = shard_levels(key, dims, pieces, -0.22, 0.18) * entries
    return jnp.clip(entries, min=-bound, max=bound).astype(kind)


def setup_inputs(seed: int = 0) -> dict:
    key_list = jax.random.split(jax.random.key(seed), 12)
    return {
        "hidden": normal_values(key_list[0], (N_GROUP * BLOCK, D), 1.0, 6.0, ((0, 32), (1, 16))),
        "w_kv": normal_values(key_list[1], (D, 2 * KVH * HD), D ** -0.5, 0.0625, ((0, 16),)),
        "prompt_lengths": jax.vmap(lambda own: uneven_parts(own, PROMPTS, BLOCK, MAXLEN, 2))(jax.random.split(key_list[2], PREFILL)).reshape((PREFILL, PROMPTS)).astype(jnp.int32),
        "owner_step": touch_ends(jax.random.randint(key_list[3], (PREFILL, PROMPTS), 1, 4), jax.random.fold_in(key_list[3], 1), 1, 3).astype(jnp.int32),
        "cache": draw_cache(jax.random.fold_in(key_list[11], 71), 0),
        "cache_len": touch_ends(jax.random.randint(key_list[5], (N_GROUP * REQUESTS,), 1, CACHE + 1), jax.random.fold_in(key_list[5], 1), 1, CACHE).astype(jnp.int32),
        "queries": draw_queries(jax.random.fold_in(key_list[11], 71), 0),
        "fresh": draw_fresh(jax.random.fold_in(key_list[11], 71), 0),
        "logits": draw_logits(jax.random.fold_in(key_list[11], 71), 0),
        "states": touch_ends(jax.random.randint(key_list[9], (N_GROUP * REQUESTS,), 0, STATES), jax.random.fold_in(key_list[9], 1), 0, STATES - 1).astype(jnp.int32),
        "masks": draw_masks(jax.random.fold_in(key_list[11], 71), 0),
    }


def landing(slot_ids, source, turn_index, prompt_lengths, owner_step):
    chosen = owner_step[source] == turn_index
    ranking = jnp.cumsum(chosen.astype(jnp.int32)) - 1
    arrivals = jnp.sum(chosen.astype(jnp.int32))
    matched = chosen[None, :] & (ranking[None, :] == slot_ids[:, None])
    lengths = prompt_lengths[source]
    starts = jnp.cumsum(lengths) - lengths
    first_row = lax.optimization_barrier(jnp.sum(jnp.where(matched, starts[None, :], 0), axis=1)).astype(jnp.int32)
    prompt_len = lax.optimization_barrier(jnp.sum(jnp.where(matched, lengths[None, :], 0), axis=1)).astype(jnp.int32)
    landed = (slot_ids < arrivals) & (turn_index >= 1)
    return (landed, first_row, prompt_len)

def attend(query_rows, merged, alive_len, fresh_rows):
    row_count = merged.shape[0]
    group_size = HEADS // KVH
    key_rows = merged[:, :, :KVH * HD].astype(jnp.float32).reshape(row_count, CACHE, KVH, HD)
    value_rows = merged[:, :, KVH * HD:].astype(jnp.float32).reshape(row_count, CACHE, KVH, HD)
    queries = query_rows.astype(jnp.float32).reshape(row_count, KVH, group_size, HD)
    own_key = fresh_rows[:, :KVH * HD].astype(jnp.float32).reshape(row_count, KVH, HD)
    own_value = fresh_rows[:, KVH * HD:].astype(jnp.float32).reshape(row_count, KVH, HD)
    scaling = 1.0 / math.sqrt(HD)
    scores = jnp.einsum('rkgd,rtkd->rkgt', queries, key_rows) * scaling
    own_score = jnp.einsum('rkgd,rkd->rkg', queries, own_key) * scaling
    positions = jnp.arange(CACHE, dtype=jnp.int32)
    alive_mask = (positions[None, :] < alive_len[:, None])[:, None, None, :]
    highest = jnp.maximum(lax.optimization_barrier(jnp.max(jnp.where(alive_mask, scores, -jnp.inf), axis=3)), own_score)
    exponent = jnp.where(alive_mask, jnp.exp(scores - highest[..., None]), 0.0)
    own_exponent = jnp.exp(own_score - highest)
    denominator = lax.optimization_barrier(jnp.sum(exponent, axis=3)) + own_exponent
    weights = lax.optimization_barrier((exponent / denominator[..., None]).astype(jnp.bfloat16)).astype(jnp.float32)
    own_weight = lax.optimization_barrier((own_exponent / denominator).astype(jnp.bfloat16)).astype(jnp.float32)
    attended = jnp.einsum('rkgt,rtkd->rkgd', weights, value_rows)
    attended = attended + own_weight[..., None] * own_value[:, :, None, :]
    return attended.reshape(row_count, HEADS * HD).astype(jnp.bfloat16)

def reference(hidden, w_kv, prompt_lengths, owner_step, cache, cache_len, queries, fresh, logits, states, masks):
    blocks = hidden.reshape(N_GROUP, BLOCK, D)[:PREFILL]
    projected = lax.map(lambda hidden_block: jnp.dot(hidden_block, w_kv, preferred_element_type=jnp.float32).astype(jnp.bfloat16), blocks)
    padded = jnp.pad(projected, ((0, 0), (0, MAXLEN), (0, 0)))
    local_ids = jnp.arange(REQUESTS, dtype=jnp.int32)
    slot_ids = local_ids % REQ_DEV * N_TP + local_ids // REQ_DEV

    def decode_group(items):
        group_index, cache_rows, alive_len, query_rows, fresh_rows = items
        source = group_index % PREFILL
        turn_index = group_index // PREFILL
        landed, first_row, prompt_len = landing(slot_ids, source, turn_index, prompt_lengths, owner_step)
        source_rows = padded[source]
        handed = jax.vmap(lambda offset: lax.dynamic_slice_in_dim(source_rows, offset, MAXLEN, 0))(first_row)
        front = jnp.where(landed[:, None, None], handed, cache_rows[:, :MAXLEN])
        merged = jnp.concatenate([front, cache_rows[:, MAXLEN:]], axis=1)
        alive = jnp.where(landed, prompt_len, alive_len)
        return attend(query_rows, merged, alive, fresh_rows)
    attended = lax.map(decode_group, (jnp.arange(N_GROUP, dtype=jnp.int32), cache.reshape(N_GROUP, REQUESTS, CACHE, 2 * KVH * HD), cache_len.reshape(N_GROUP, REQUESTS), queries.reshape(N_GROUP, REQUESTS, HEADS * HD), fresh.reshape(N_GROUP, REQUESTS, 2 * KVH * HD)))
    attended = attended.reshape(N_GROUP * REQUESTS, HEADS * HD)

    def grammar_rows(items):
        logit_rows, state_ids = items
        packed = masks[state_ids]
        shifts = jnp.arange(30, dtype=jnp.int32)
        bit_flags = jnp.bitwise_and(jnp.right_shift(packed[:, :, None], shifts[None, None, :]), 1)
        permitted = bit_flags.reshape(packed.shape[0], VOCAB) == 1
        values = logit_rows.astype(jnp.float32)
        highest = lax.optimization_barrier(jnp.max(jnp.where(permitted, values, -jnp.inf), axis=1))
        denominator = lax.optimization_barrier(jnp.sum(jnp.where(permitted, jnp.exp(values - highest[:, None]), 0.0), axis=1))
        normalizer = highest + jnp.log(denominator)
        return jnp.where(permitted, values - normalizer[:, None], 0.0)
    logprob = lax.map(grammar_rows, (logits.reshape(N_GROUP, REQUESTS, VOCAB), states.reshape(N_GROUP, REQUESTS)))
    return (attended, logprob.reshape(N_GROUP * REQUESTS, VOCAB))
```

```python
import math

import jax
import jax.numpy as jnp
from jax import lax
from jax.experimental import pallas as pl
from jax.experimental.pallas import tpu as pltpu
from jax.sharding import Mesh, PartitionSpec as P

HEADS = 64
KVH = 8
HD = 128
STATES = 24
BITS = 30
BLK = 1920
SCALE = 1.0 / math.sqrt(HD)
F32 = jnp.float32
BF16 = jnp.bfloat16
I32 = jnp.int32
TP = ("zh", "zl")


def iota(shape, dim):
    return lax.broadcasted_iota(I32, shape, dim)


def one_hot(target, width):
    rows = target.shape[0]
    return (iota((rows, width), 1) == target).astype(F32).astype(BF16)


def pick(target, table):
    return jnp.dot(one_hot(target, table.shape[0]), table, preferred_element_type=F32)


def call(kernel, out, name, memory=None):
    return pl.pallas_call(kernel, out_shape=out, name=name)


def prompts_of(lengths, owners, source, turn):
    count = lengths.shape[1]
    here = iota(lengths.shape, 0) == source
    length = jnp.sum(jnp.where(here, lengths, 0).astype(F32), axis=0, keepdims=True)
    owner = jnp.sum(jnp.where(here, owners, 0).astype(F32), axis=0, keepdims=True)
    chosen = ((owner == turn.astype(F32)) & (turn >= 1)).astype(F32)
    row, lane = iota((count, count), 0), iota((count, count), 1)

    def before(values):
        column = jnp.sum(jnp.where(row == lane, values, 0.0), axis=1, keepdims=True)
        return jnp.sum(jnp.where(row < lane, column, 0.0), axis=0, keepdims=True)

    return chosen, before(chosen), before(length), length


def landing(slot, prompts):
    chosen, rank, start, length = prompts
    matched = jnp.where(rank == slot.astype(F32), chosen, 0.0)
    total = lambda values: jnp.sum(matched * values, axis=1, keepdims=True)
    return jnp.sum(matched, axis=1, keepdims=True), total(start), total(length)


def pack_queries(queries, fresh, out):
    table = jnp.concatenate(
        [queries[:, HD * i : HD * (i + 1)] for i in range(4)] + [fresh[...]], axis=0
    )
    row = iota((256, 1), 0)
    dest, k = row // 16, row % 16
    target = jnp.where(
        k < 8,
        (k % 4) * 32 + 2 * dest + k // 4,
        jnp.where(k < 10, 128 + 2 * dest + k - 8, 160),
    )
    out[...] = pick(target, table).astype(BF16).reshape(16, 16, HD)


def project(own, first, second, third, weight, out):
    turn = lax.axis_index("x")
    tokens = jnp.where(turn == 0, own[0:64, :], first[...] + second[...] + third[...])
    full = jnp.dot(tokens, weight[...], preferred_element_type=F32).astype(BF16)
    for c in range(16):
        block = c // 2 + (c % 2) * KVH
        out[c] = full[:, HD * block : HD * (block + 1)]


def reduce_blocks(pieces, out):
    total = pieces[0].astype(F32)
    for c in range(1, 16):
        total = total + pieces[c].astype(F32)
    total = total.astype(BF16)
    for d in range(8):
        out[d] = total


def grammar(logits, key, masks, masked, terms):
    lane = iota((STATES, HD), 1)
    blocks = []
    for half in range(2):
        words = masks[:, HD * half : HD * (half + 1)]
        turned = pltpu.roll(words, 64, 1)
        for x, y in ((words, turned), (turned, words)):
            byte = lambda v, j: jnp.bitwise_and(jnp.right_shift(v, 8 * j), 255)
            blocks.append(
                jnp.concatenate(
                    [
                        jnp.where(lane < 64, byte(x, 0), byte(y, 1)),
                        jnp.where(lane < 64, byte(x, 2), byte(y, 3)),
                    ],
                    axis=1,
                )
            )
    table = jnp.concatenate(blocks, axis=0).astype(F32).astype(BF16)
    chosen = pick(key[...], table).astype(BF16)
    column = iota((1, BLK), 1)
    word = jnp.right_shift(column * 34953, 20)
    bit = column - word * BITS
    wanted = jnp.right_shift(bit, 3) * 64 + word
    flag = jnp.left_shift(jnp.ones_like(bit), jnp.bitwise_and(bit, 7))
    spread = (iota((256, BLK), 0) == wanted).astype(F32).astype(BF16)
    peak = None
    kept = []
    for b in range(4):
        value = jnp.dot(
            chosen[32 * b : 32 * (b + 1)], spread, preferred_element_type=F32
        ).astype(I32)
        section = logits[:, BLK * b : BLK * (b + 1)].astype(F32)
        section = jnp.where(jnp.bitwise_and(value, flag) != 0, section, -jnp.inf)
        kept.append(section)
        masked[:, BLK * b : BLK * (b + 1)] = section.astype(BF16)
        top = jnp.max(section, axis=1, keepdims=True)
        peak = top if peak is None else jnp.maximum(peak, top)
    total = sum(jnp.sum(jnp.exp(section - peak), axis=1, keepdims=True) for section in kept)
    high = total.astype(BF16).astype(F32)
    middle = (total - high).astype(BF16).astype(F32)
    low = total - high - middle
    row, lane = iota((32, HD), 0), iota((32, HD), 1)
    spot = lane - row
    line = jnp.where(
        spot == 0, peak, jnp.where(spot == 32, high, jnp.where(spot == 64, middle, low))
    )
    line = jnp.where(jnp.bitwise_and(spot, 31) == 0, line, 0.0)
    terms[...] = jnp.broadcast_to(jnp.sum(line, axis=0, keepdims=True), (16, HD)).astype(BF16)


def softmax(score, own, alive):
    highest = jnp.maximum(
        jnp.max(jnp.where(alive, score, -jnp.inf), axis=1, keepdims=True), own
    )
    exponent = jnp.where(alive, jnp.exp(score - highest), 0.0)
    own_exponent = jnp.exp(own - highest)
    total = jnp.sum(exponent, axis=1, keepdims=True) + own_exponent
    own_weight = (own_exponent / total).astype(BF16).astype(F32)
    return (exponent / total).astype(BF16), own_weight


def transposed(a, b):
    return lax.dot_general(a, b, (((1,), (1,)), ((), ())), preferred_element_type=F32)


def attend_cached(cache_len, received, cache, terms, lengths, owners, out):
    column = lax.axis_index("zh") * 2 + lax.axis_index("zl")
    prompts = prompts_of(
        lengths[...], owners[...], lax.axis_index("c8"), lax.axis_index("x")
    )
    landed = landing(jnp.full((1, 1), column, I32), prompts)[0]
    table = received[...].reshape(256, HD)
    row = iota((256, 1), 0)
    device, k = row // 16, row % 16
    second = (k >= 4) & (k < 8)
    fresh_row = (device // 2) * 16 + jnp.where(second, 9, 8)
    own_key = pick(fresh_row, table)
    own_value = pick(fresh_row + KVH * 16, table)
    own = jnp.sum(table.astype(F32) * own_key, axis=1, keepdims=True) * SCALE
    second32 = second[0:32]
    scores = []
    for h in range(KVH):
        rows = table[32 * h : 32 * (h + 1)]
        both = [transposed(rows, cache[r, :, HD * h : HD * (h + 1)]) for r in range(2)]
        scores.append(jnp.where(second32, both[1], both[0]))
    score = jnp.concatenate(scores, axis=0) * SCALE
    alive = iota((256, HD), 1) < jnp.where(second, cache_len[1], cache_len[0])
    weight, own_weight = softmax(score, own, alive)
    values = []
    for h in range(KVH):
        rows = weight[32 * h : 32 * (h + 1)]
        at = HD * (KVH + h)
        both = [
            jnp.dot(rows, cache[r, :, at : at + HD], preferred_element_type=F32)
            for r in range(2)
        ]
        values.append(jnp.where(second32, both[1], both[0]))
    result = jnp.concatenate(values, axis=0) + own_weight * own_value
    arrived = jnp.broadcast_to(landed > 0.5, (256, 1))
    result = jnp.where(arrived & (k == 0), own_key, result)
    result = jnp.where(arrived & (k == 1), own_value, result)
    result = jnp.where(k == 8, terms[0:1, :].astype(F32), result)
    out[...] = result.astype(BF16).reshape(16, 16, HD)


def finish_logprob(masked, received, out):
    lines = received[:, 8, :].astype(F32)
    take = lambda k: lines[:, 32 * k : 32 * (k + 1)]
    peak, total = take(0), take(1) + take(2) + take(3)
    highest = jnp.max(peak, axis=0, keepdims=True)
    total = jnp.sum(total * jnp.exp(peak - highest), axis=0, keepdims=True)
    normalizer = highest + jnp.log(total)
    row, lane = iota((32, 32), 0), iota((32, 32), 1)
    normalizer = jnp.sum(jnp.where(row == lane, normalizer, 0.0), axis=1, keepdims=True)
    values = masked[...].astype(F32)
    out[...] = jnp.where(values == -jnp.inf, 0.0, values - normalizer)


def attend_landed(blocks, queries, received, lengths, owners, out):
    prompts = prompts_of(
        lengths[...], owners[...], lax.axis_index("c8"), lax.axis_index("x")
    )
    row = iota((128, 1), 0)
    head, request = row // 32, row % 32
    landed, start, length = landing((request % 2) * 16 + request // 2, prompts)
    keys = jnp.concatenate([blocks[2 * x] for x in range(4)], axis=0)
    values = jnp.concatenate([blocks[2 * x + 1] for x in range(4)], axis=0)
    query = jnp.concatenate([queries[:, HD * i : HD * (i + 1)] for i in range(4)], axis=0)
    table = received[...].reshape(256, HD)
    slot = (request // 2) * 16
    own_key = pick(slot, table)
    own_value = pick(slot + 1, table)
    cached = pick(slot + (request % 2) * 4 + head, table)
    own = jnp.sum(query.astype(F32) * own_key, axis=1, keepdims=True) * SCALE
    score = transposed(query, keys) * SCALE
    position = iota((128, 256), 1).astype(F32)
    alive = (position >= start) & (position < start + length)
    weight, own_weight = softmax(score, own, alive)
    result = jnp.dot(weight, values, preferred_element_type=F32) + own_weight * own_value
    result = jnp.where(landed > 0.5, result, cached).astype(BF16)
    for i in range(4):
        out[:, HD * i : HD * (i + 1)] = result[32 * i : 32 * (i + 1)]


def exchanged(slots, axis):
    return lax.all_to_all(slots, axis, 0, 0, tiled=True)


def per_device(
    hidden,
    w_kv,
    prompt_lengths,
    owner_step,
    cache,
    cache_len,
    queries,
    fresh,
    logits,
    states,
    masks,
):
    shape = jax.ShapeDtypeStruct
    smem = pl.BlockSpec(memory_space=pltpu.SMEM)
    vmem = pl.BlockSpec(memory_space=pltpu.VMEM)
    shares = [
        lax.ppermute(hidden[64 * k : 64 * (k + 1)], "x", [(0, k)]) for k in (1, 2, 3)
    ]
    asked = pl.pallas_call(pack_queries, out_shape=shape((16, 16, HD), BF16), name="pack")(
        queries, fresh
    )
    asked = exchanged(asked, TP)
    projected = pl.pallas_call(
        project, out_shape=shape((16, 64, HD), BF16), name="project"
    )(hidden[0:64], *shares, w_kv)
    pieces = exchanged(projected, TP)
    key = (states[None, :] + STATES * jnp.arange(4, dtype=I32)[:, None]).reshape(128, 1)
    masked, terms = pl.pallas_call(
        grammar,
        out_shape=(shape(logits.shape, BF16), shape((16, HD), BF16)),
        name="grammar",
    )(logits, key, masks)
    answers = pl.pallas_call(
        attend_cached,
        out_shape=shape((16, 16, HD), BF16),
        in_specs=[smem] + [vmem] * 5,
        name="cached",
    )(cache_len, asked, cache, terms, prompt_lengths, owner_step)
    answers = exchanged(answers, TP)
    blocks = pl.pallas_call(
        reduce_blocks, out_shape=shape((8, 64, HD), BF16), name="reduce"
    )(pieces)
    blocks = exchanged(blocks, ("x", "zl"))
    logprob = pl.pallas_call(
        finish_logprob, out_shape=shape(logits.shape, F32), name="logprob"
    )(masked, answers)
    attended = pl.pallas_call(
        attend_landed, out_shape=shape(queries.shape, BF16), name="landed"
    )(blocks, queries, answers, prompt_lengths, owner_step)
    return attended, logprob


def solution(mesh):
    groups, columns = mesh.shape["group"], mesh.shape["tp"]
    finer = Mesh(
        mesh.devices.reshape(4, groups // 4, columns // 2, 2), ("x", "c8", "zh", "zl")
    )
    group = ("x", "c8")
    in_specs = (
        P(group, TP),
        P(TP, None),
        P(),
        P(),
        P(group + TP, None, None),
        P(group + TP),
        P(group, TP),
        P(group, TP),
        P(group, TP),
        P(group),
        P(None, TP),
    )
    return jax.shard_map(
        per_device,
        mesh=finer,
        in_specs=in_specs,
        out_specs=(P(group, TP), P(group, TP)),
        check_vma=False,
    )
```

```python
import math

import jax
import jax.numpy as jnp
from jax import lax
from jax.experimental import pallas as pl
from jax.experimental.pallas import tpu as pltpu
from jax.sharding import Mesh, PartitionSpec as P

KVH = 8
HD = 128
STATES = 24
BITS = 30
LOWEST = -1e30
BLK = 1920
SCALE = 1.0 / math.sqrt(HD)
F32 = jnp.float32
BF16 = jnp.bfloat16
I32 = jnp.int32
TP = ("zh", "zl")


def iota(shape, dim):
    return lax.broadcasted_iota(I32, shape, dim)


def one_hot(target, width):
    rows = target.shape[0]
    return (iota((rows, width), 1) == target).astype(F32).astype(BF16)


def pick(target, table):
    return jnp.dot(one_hot(target, table.shape[0]), table, preferred_element_type=F32)


def prompts_of(lengths, owners, source, turn):
    count = lengths.shape[1]
    here = iota(lengths.shape, 0) == source
    length = jnp.sum(jnp.where(here, lengths, 0).astype(F32), axis=0, keepdims=True)
    owner = jnp.sum(jnp.where(here, owners, 0).astype(F32), axis=0, keepdims=True)
    chosen = ((owner == turn.astype(F32)) & (turn >= 1)).astype(F32)
    row, lane = iota((count, count), 0), iota((count, count), 1)

    def before(values):
        column = jnp.sum(jnp.where(row == lane, values, 0.0), axis=1, keepdims=True)
        return jnp.sum(jnp.where(row < lane, column, 0.0), axis=0, keepdims=True)

    return chosen, before(chosen), before(length), length


def landing(slot, prompts):
    chosen, rank, start, length = prompts
    matched = jnp.where(rank == slot.astype(F32), chosen, 0.0)
    total = lambda values: jnp.sum(matched * values, axis=1, keepdims=True)
    return jnp.sum(matched, axis=1, keepdims=True), total(start), total(length)


def prepare(hidden, queries, fresh, own, first, second, third, asked, query, new, sems):
    shares = [
        pltpu.make_async_copy(hidden.at[pl.ds(64 * k, 64)], out, sems.at[k])
        for k, out in enumerate((own, first, second, third))
    ]
    loads = [
        pltpu.make_async_copy(queries, query, sems.at[4]),
        pltpu.make_async_copy(fresh, new, sems.at[5]),
    ]
    for copy in loads + shares:
        copy.start()
    for copy in loads:
        copy.wait()
    table = jnp.concatenate(
        [query[:, HD * i : HD * (i + 1)] for i in range(4)] + [new[...]], axis=0
    )
    row = iota((256, 1), 0)
    dest, k = row // 16, row % 16
    target = jnp.where(
        k < 8,
        (k % 4) * 32 + 2 * dest + k // 4,
        jnp.where(k < 10, 128 + 2 * dest + k - 8, 160),
    )
    asked[...] = pick(target, table).astype(BF16).reshape(16, 16, HD)
    for copy in shares:
        copy.wait()


def fetch(weight, out, sem):
    copy = pltpu.make_async_copy(weight, out, sem)
    copy.start()
    copy.wait()


def project(own, first, second, third, weight, asked, out):
    turn = lax.axis_index("x")
    tokens = jnp.where(turn == 0, own[...], first[...] + second[...] + third[...])
    full = jnp.dot(tokens, weight[...], preferred_element_type=F32).astype(BF16)
    for c in range(16):
        block = c // 2 + (c % 2) * KVH
        out[c, 0:64] = full[:, HD * block : HD * (block + 1)]
        out[c, 64:80] = asked[c]


def reduce_blocks(pieces, out):
    total = pieces[0, 0:64].astype(F32)
    for c in range(1, 16):
        total = total + pieces[c, 0:64].astype(F32)
    total = total.astype(BF16)
    for d in range(8):
        out[d] = total


def grammar(logits, states, masks, masked, terms):
    lane = iota((STATES, HD), 1)
    blocks = []
    for half in range(2):
        words = masks[:, HD * half : HD * (half + 1)]
        turned = pltpu.roll(words, 64, 1)
        for x, y in ((words, turned), (turned, words)):
            byte = lambda v, j: jnp.bitwise_and(jnp.right_shift(v, 8 * j), 255)
            blocks.append(
                jnp.concatenate(
                    [
                        jnp.where(lane < 64, byte(x, 0), byte(y, 1)),
                        jnp.where(lane < 64, byte(x, 2), byte(y, 3)),
                    ],
                    axis=1,
                )
            )
    table = jnp.concatenate(blocks, axis=0).astype(F32).astype(BF16)
    row, lane = iota((32, 32), 0), iota((32, 32), 1)
    state = jnp.where(row == lane, states[...], 0).astype(F32)
    state = jnp.sum(state, axis=1, keepdims=True).astype(I32)
    key = jnp.concatenate([state + STATES * b for b in range(4)], axis=0)
    chosen = pick(key, table).astype(BF16)
    column = iota((1, BLK), 1)
    word = jnp.right_shift(column * 34953, 20)
    bit = column - word * BITS
    wanted = jnp.right_shift(bit, 3) * 64 + word
    flag = jnp.left_shift(jnp.ones_like(bit), jnp.bitwise_and(bit, 7))
    spread = (iota((256, BLK), 0) == wanted).astype(F32).astype(BF16)
    peak = None
    kept = []
    for b in range(4):
        value = jnp.dot(
            chosen[32 * b : 32 * (b + 1)], spread, preferred_element_type=F32
        ).astype(I32)
        section = logits[:, BLK * b : BLK * (b + 1)].astype(F32)
        section = jnp.where(jnp.bitwise_and(value, flag) != 0, section, -jnp.inf)
        kept.append(section)
        masked[:, BLK * b : BLK * (b + 1)] = section.astype(BF16)
        top = jnp.max(section, axis=1, keepdims=True)
        peak = top if peak is None else jnp.maximum(peak, top)
    total = sum(jnp.sum(jnp.exp(section - peak), axis=1, keepdims=True) for section in kept)
    high = total.astype(BF16).astype(F32)
    middle = (total - high).astype(BF16).astype(F32)
    low = total - high - middle
    row, lane = iota((32, HD), 0), iota((32, HD), 1)
    spot = lane - row
    line = jnp.where(
        spot == 0, peak, jnp.where(spot == 32, high, jnp.where(spot == 64, middle, low))
    )
    line = jnp.where(jnp.bitwise_and(spot, 31) == 0, line, 0.0)
    terms[...] = jnp.broadcast_to(jnp.sum(line, axis=0, keepdims=True), (16, HD)).astype(BF16)


def softmax(score, own, alive):
    highest = jnp.maximum(
        jnp.max(jnp.where(alive, score, -jnp.inf), axis=1, keepdims=True), own
    )
    exponent = jnp.where(alive, jnp.exp(score - highest), 0.0)
    own_exponent = jnp.exp(own - highest)
    total = jnp.sum(exponent, axis=1, keepdims=True) + own_exponent
    own_weight = (own_exponent / total).astype(BF16).astype(F32)
    return (exponent / total).astype(BF16), own_weight


def transposed(a, b):
    return lax.dot_general(a, b, (((1,), (1,)), ((), ())), preferred_element_type=F32)


def attend_cached(cache_len, received, cache, terms, lengths, owners, out):
    column = lax.axis_index("zh") * 2 + lax.axis_index("zl")
    prompts = prompts_of(
        lengths[...], owners[...], lax.axis_index("c8"), lax.axis_index("x")
    )
    landed = landing(jnp.full((1, 1), column, I32), prompts)[0]
    table = received[:, 64:80, :].reshape(256, HD)
    row = iota((256, 1), 0)
    device, k = row // 16, row % 16
    second = (k >= 4) & (k < 8)
    fresh_row = (device // 2) * 16 + jnp.where(second, 9, 8)
    own_key = pick(fresh_row, table)
    own_value = pick(fresh_row + KVH * 16, table)
    own = jnp.sum(table.astype(F32) * own_key, axis=1, keepdims=True) * SCALE
    second32 = second[0:32]
    scores = []
    for h in range(KVH):
        rows = table[32 * h : 32 * (h + 1)]
        both = [transposed(rows, cache[r, :, HD * h : HD * (h + 1)]) for r in range(2)]
        scores.append(jnp.where(second32, both[1], both[0]))
    score = jnp.concatenate(scores, axis=0) * SCALE
    alive = iota((256, HD), 1) < jnp.where(second, cache_len[1], cache_len[0])
    weight, own_weight = softmax(score, own, alive)
    values = []
    for h in range(KVH):
        rows = weight[32 * h : 32 * (h + 1)]
        at = HD * (KVH + h)
        both = [
            jnp.dot(rows, cache[r, :, at : at + HD], preferred_element_type=F32)
            for r in range(2)
        ]
        values.append(jnp.where(second32, both[1], both[0]))
    result = jnp.concatenate(values, axis=0) + own_weight * own_value
    arrived = jnp.broadcast_to(landed > 0.5, (256, 1))
    result = jnp.where(arrived & (k == 0), own_key, result)
    result = jnp.where(arrived & (k == 1), own_value, result)
    result = jnp.where(k == 8, terms[0:1, :].astype(F32), result)
    out[...] = result.astype(BF16).reshape(16, 16, HD)


def own_prompts(row, lengths, owners):
    request = row % 32
    prompts = prompts_of(
        lengths[...], owners[...], lax.axis_index("c8"), lax.axis_index("x")
    )
    return landing((request % 2) * 16 + request // 2, prompts)


def attend_prompts(blocks, queries, lengths, owners, result, stats):
    row = iota((128, 1), 0)
    landed, start, length = own_prompts(row, lengths, owners)
    keys = jnp.concatenate([blocks[2 * x] for x in range(4)], axis=0)
    values = jnp.concatenate([blocks[2 * x + 1] for x in range(4)], axis=0)
    query = jnp.concatenate([queries[:, HD * i : HD * (i + 1)] for i in range(4)], axis=0)
    score = transposed(query, keys) * SCALE
    position = iota((128, 256), 1).astype(F32)
    alive = (position >= start) & (position < start + length)
    highest = jnp.max(jnp.where(alive, score, LOWEST), axis=1, keepdims=True)
    exponent = jnp.where(alive, jnp.exp(score - highest), 0.0)
    result[...] = jnp.dot(exponent.astype(BF16), values, preferred_element_type=F32)
    total = jnp.sum(exponent, axis=1, keepdims=True)
    lane = iota((128, HD), 1)
    stats[...] = jnp.where(lane == 0, highest, jnp.where(lane == 1, total, landed))


def finish(masked, received, queries, result, stats, logprob, attended, values, sems):
    lines = received[:, 8, :].astype(F32)
    take = lambda k: lines[:, 32 * k : 32 * (k + 1)]
    peak, total = take(0), take(1) + take(2) + take(3)
    highest = jnp.max(peak, axis=0, keepdims=True)
    total = jnp.sum(total * jnp.exp(peak - highest), axis=0, keepdims=True)
    normalizer = highest + jnp.log(total)
    row, lane = iota((32, 32), 0), iota((32, 32), 1)
    normalizer = jnp.sum(jnp.where(row == lane, normalizer, 0.0), axis=1, keepdims=True)
    copies = []
    for b in range(4):
        at = slice(BLK * b, BLK * (b + 1))
        section = masked[:, at].astype(F32)
        values[:, at] = jnp.where(section == -jnp.inf, 0.0, section - normalizer)
        copies.append(
            pltpu.make_async_copy(
                values.at[:, pl.ds(BLK * b, BLK)], logprob.at[:, pl.ds(BLK * b, BLK)], sems.at[b]
            )
        )
        copies[-1].start()
    row = iota((128, 1), 0)
    head, request = row // 32, row % 32
    query = jnp.concatenate([queries[:, HD * i : HD * (i + 1)] for i in range(4)], axis=0)
    table = received[...].reshape(256, HD)
    slot = (request // 2) * 16
    own_key = pick(slot, table)
    own_value = pick(slot + 1, table)
    cached = pick(slot + (request % 2) * 4 + head, table)
    own = jnp.sum(query.astype(F32) * own_key, axis=1, keepdims=True) * SCALE
    top, total, landed = stats[:, 0:1], stats[:, 1:2], stats[:, 2:3]
    highest = jnp.maximum(top, own)
    share, own_share = jnp.exp(top - highest), jnp.exp(own - highest)
    scale = 1.0 / (total * share + own_share)
    merged = (result[...] * share + own_value * own_share) * scale
    merged = jnp.where(landed > 0.5, merged, cached).astype(BF16)
    for i in range(4):
        attended[:, HD * i : HD * (i + 1)] = merged[32 * i : 32 * (i + 1)]
    for copy in copies:
        copy.wait()


def exchanged(slots, axis):
    return lax.all_to_all(slots, axis, 0, 0, tiled=True)


def per_device(
    hidden,
    w_kv,
    prompt_lengths,
    owner_step,
    cache,
    cache_len,
    queries,
    fresh,
    logits,
    states,
    masks,
):
    smem = pl.BlockSpec(memory_space=pltpu.SMEM)
    vmem = pl.BlockSpec(memory_space=pltpu.VMEM)
    hbm = pl.BlockSpec(memory_space=pl.ANY)
    sent = jax.ShapeDtypeStruct
    kept = pltpu.VMEM
    held = lambda *values: [
        pltpu.with_memory_space_constraint(value, pltpu.VMEM) for value in values
    ]
    tokens, wide = hidden.shape[0] // 4, hidden.shape[1]
    *shares, asked = pl.pallas_call(
        prepare,
        out_shape=[kept((tokens, wide), BF16)] * 4 + [kept((16, 16, HD), BF16)],
        in_specs=[hbm] * 3,
        out_specs=[vmem] * 5,
        scratch_shapes=[
            pltpu.VMEM(queries.shape, BF16),
            pltpu.VMEM(fresh.shape, BF16),
            pltpu.SemaphoreType.DMA((6,)),
        ],
        name="prepare",
    )(hidden, queries, fresh)
    shares[1:] = [lax.ppermute(shares[k], "x", [(0, k)]) for k in (1, 2, 3)]
    weight = pl.pallas_call(
        fetch,
        out_shape=kept(w_kv.shape, BF16),
        in_specs=[hbm],
        out_specs=vmem,
        scratch_shapes=[pltpu.SemaphoreType.DMA],
        name="fetch",
    )(w_kv)
    projected = pl.pallas_call(
        project,
        out_shape=sent((16, 80, HD), BF16),
        in_specs=[vmem] * 6,
        name="project",
    )(*held(*shares, weight, asked))
    pieces = exchanged(projected, TP)
    masked, terms = pl.pallas_call(
        grammar,
        out_shape=[kept(logits.shape, BF16), kept((16, HD), BF16)],
        in_specs=[vmem] * 3,
        out_specs=[vmem] * 2,
        name="grammar",
    )(*held(logits, states.reshape(1, -1), masks))
    blocks = pl.pallas_call(
        reduce_blocks,
        out_shape=sent((8, tokens, HD), BF16),
        in_specs=[vmem],
        name="reduce",
    )(*held(pieces))
    blocks = exchanged(blocks, ("x", "zl"))
    answers = pl.pallas_call(
        attend_cached,
        out_shape=sent((16, 16, HD), BF16),
        in_specs=[smem] + [vmem] * 5,
        name="cached",
    )(cache_len, *held(pieces, cache, terms, prompt_lengths, owner_step))
    answers = exchanged(answers, TP)
    result, stats = pl.pallas_call(
        attend_prompts,
        out_shape=[kept((128, HD), F32), kept((128, HD), F32)],
        in_specs=[vmem] * 4,
        out_specs=[vmem] * 2,
        name="prompts",
    )(*held(blocks, queries, prompt_lengths, owner_step))
    logprob, attended = pl.pallas_call(
        finish,
        out_shape=[sent(logits.shape, F32), sent(queries.shape, BF16)],
        in_specs=[vmem] * 5,
        out_specs=[hbm, vmem],
        scratch_shapes=[pltpu.VMEM(logits.shape, F32), pltpu.SemaphoreType.DMA((4,))],
        name="finish",
    )(*held(masked, answers, queries, result, stats))
    return attended, logprob


def solution(mesh):
    groups, columns = mesh.shape["group"], mesh.shape["tp"]
    finer = Mesh(
        mesh.devices.reshape(4, groups // 4, columns // 2, 2), ("x", "c8", "zh", "zl")
    )
    group = ("x", "c8")
    in_specs = (
        P(group, TP),
        P(TP, None),
        P(),
        P(),
        P(group + TP, None, None),
        P(group + TP),
        P(group, TP),
        P(group, TP),
        P(group, TP),
        P(group),
        P(None, TP),
    )
    return jax.shard_map(
        per_device,
        mesh=finer,
        in_specs=in_specs,
        out_specs=(P(group, TP), P(group, TP)),
        check_vma=False,
    )
```

```python
import math

import jax
import jax.numpy as jnp
from jax import lax
from jax.experimental import pallas as pl
from jax.experimental.pallas import tpu as pltpu
from jax.sharding import Mesh, PartitionSpec as P

KVH = 8
HD = 128
STATES = 24
BITS = 30
BLK = 1920
SCALE = 1.0 / math.sqrt(HD)
F32 = jnp.float32
BF16 = jnp.bfloat16
I32 = jnp.int32
TP = ("zh", "zl")


def iota(shape, dim):
    return lax.broadcasted_iota(I32, shape, dim)


def one_hot(target, width):
    rows = target.shape[0]
    return (iota((rows, width), 1) == target).astype(F32).astype(BF16)


def pick(target, table):
    return jnp.dot(one_hot(target, table.shape[0]), table, preferred_element_type=F32)


def prompts_of(lengths, owners, source, turn):
    count = lengths.shape[1]
    here = iota(lengths.shape, 0) == source
    length = jnp.sum(jnp.where(here, lengths, 0).astype(F32), axis=0, keepdims=True)
    owner = jnp.sum(jnp.where(here, owners, 0).astype(F32), axis=0, keepdims=True)
    chosen = ((owner == turn.astype(F32)) & (turn >= 1)).astype(F32)
    row, lane = iota((count, count), 0), iota((count, count), 1)

    def before(values):
        column = jnp.sum(jnp.where(row == lane, values, 0.0), axis=1, keepdims=True)
        return jnp.sum(jnp.where(row < lane, column, 0.0), axis=0, keepdims=True)

    return chosen, before(chosen), before(length), length


def landing(slot, prompts):
    chosen, rank, start, length = prompts
    matched = jnp.where(rank == slot.astype(F32), chosen, 0.0)
    total = lambda values: jnp.sum(matched * values, axis=1, keepdims=True)
    return jnp.sum(matched, axis=1, keepdims=True), total(start), total(length)


def prepare(hidden, queries, fresh, own, first, second, third, asked, query, new, sems):
    shares = [
        pltpu.make_async_copy(hidden.at[pl.ds(64 * k, 64)], out, sems.at[k])
        for k, out in enumerate((own, first, second, third))
    ]
    loads = [
        pltpu.make_async_copy(queries, query, sems.at[4]),
        pltpu.make_async_copy(fresh, new, sems.at[5]),
    ]
    for copy in loads + shares:
        copy.start()
    for copy in loads:
        copy.wait()
    table = jnp.concatenate(
        [query[:, HD * i : HD * (i + 1)] for i in range(4)] + [new[...]], axis=0
    )
    row = iota((256, 1), 0)
    dest, k = row // 16, row % 16
    target = jnp.where(
        k < 8,
        (k % 4) * 32 + 2 * dest + k // 4,
        jnp.where(k < 10, 128 + 2 * dest + k - 8, 160),
    )
    asked[...] = pick(target, table).astype(BF16).reshape(16, 16, HD)
    for copy in shares:
        copy.wait()


def project(own, first, second, third, asked, weight, out, held, sems):
    width = weight.shape[1] // 4
    loads = [
        pltpu.make_async_copy(
            weight.at[:, pl.ds(width * k, width)], held.at[:, pl.ds(width * k, width)], sems.at[k]
        )
        for k in range(4)
    ]
    for load in loads:
        load.start()
    turn = lax.axis_index("x")
    tokens = jnp.where(turn == 0, own[...], first[...] + second[...] + third[...])
    out[:, 64:80] = asked[...]
    for k in range(4):
        loads[k].wait()
        part = held[:, width * k : width * (k + 1)]
        part = jnp.dot(tokens, part, preferred_element_type=F32).astype(BF16)
        for i in range(4):
            block = 4 * k + i
            c = 2 * (block % KVH) + block // KVH
            out[c, 0:64] = part[:, HD * i : HD * (i + 1)]


def reduce_blocks(pieces, out):
    total = pieces[0, 0:64].astype(F32)
    for c in range(1, 16):
        total = total + pieces[c, 0:64].astype(F32)
    out[...] = total.astype(BF16)


def grammar(logits, states, masks, masked, terms):
    lane = iota((STATES, HD), 1)
    blocks = []
    for half in range(2):
        words = masks[:, HD * half : HD * (half + 1)]
        turned = pltpu.roll(words, 64, 1)
        for x, y in ((words, turned), (turned, words)):
            byte = lambda v, j: jnp.bitwise_and(jnp.right_shift(v, 8 * j), 255)
            blocks.append(
                jnp.concatenate(
                    [
                        jnp.where(lane < 64, byte(x, 0), byte(y, 1)),
                        jnp.where(lane < 64, byte(x, 2), byte(y, 3)),
                    ],
                    axis=1,
                )
            )
    table = jnp.concatenate(blocks, axis=0).astype(F32).astype(BF16)
    row, lane = iota((32, 32), 0), iota((32, 32), 1)
    state = jnp.where(row == lane, states[...], 0).astype(F32)
    state = jnp.sum(state, axis=1, keepdims=True).astype(I32)
    key = jnp.concatenate([state + STATES * b for b in range(4)], axis=0)
    chosen = pick(key, table).astype(BF16)
    column = iota((1, BLK), 1)
    word = jnp.right_shift(column * 34953, 20)
    bit = column - word * BITS
    wanted = jnp.right_shift(bit, 3) * 64 + word
    flag = jnp.left_shift(jnp.ones_like(bit), jnp.bitwise_and(bit, 7))
    spread = (iota((256, BLK), 0) == wanted).astype(F32).astype(BF16)
    peak = None
    kept = []
    for b in range(4):
        value = jnp.dot(
            chosen[32 * b : 32 * (b + 1)], spread, preferred_element_type=F32
        ).astype(I32)
        section = logits[:, BLK * b : BLK * (b + 1)].astype(F32)
        section = jnp.where(jnp.bitwise_and(value, flag) != 0, section, -jnp.inf)
        kept.append(section)
        masked[:, BLK * b : BLK * (b + 1)] = section.astype(BF16)
        top = jnp.max(section, axis=1, keepdims=True)
        peak = top if peak is None else jnp.maximum(peak, top)
    total = sum(jnp.sum(jnp.exp(section - peak), axis=1, keepdims=True) for section in kept)
    high = total.astype(BF16).astype(F32)
    middle = (total - high).astype(BF16).astype(F32)
    low = total - high - middle
    row, lane = iota((32, HD), 0), iota((32, HD), 1)
    spot = lane - row
    line = jnp.where(
        spot == 0, peak, jnp.where(spot == 32, high, jnp.where(spot == 64, middle, low))
    )
    line = jnp.where(jnp.bitwise_and(spot, 31) == 0, line, 0.0)
    terms[...] = jnp.broadcast_to(jnp.sum(line, axis=0, keepdims=True), (16, HD)).astype(BF16)


def softmax(score, own, alive):
    highest = jnp.maximum(
        jnp.max(jnp.where(alive, score, -jnp.inf), axis=1, keepdims=True), own
    )
    exponent = jnp.where(alive, jnp.exp(score - highest), 0.0)
    own_exponent = jnp.exp(own - highest)
    total = jnp.sum(exponent, axis=1, keepdims=True) + own_exponent
    own_weight = (own_exponent / total).astype(BF16).astype(F32)
    return (exponent / total).astype(BF16), own_weight


def transposed(a, b):
    return lax.dot_general(a, b, (((1,), (1,)), ((), ())), preferred_element_type=F32)


def attend_cached(cache_len, received, cache, terms, lengths, owners, out):
    column = lax.axis_index("zh") * 2 + lax.axis_index("zl")
    prompts = prompts_of(
        lengths[...], owners[...], lax.axis_index("c8"), lax.axis_index("x")
    )
    landed = landing(jnp.full((1, 1), column, I32), prompts)[0]
    table = received[:, 64:80, :].reshape(256, HD)
    row = iota((256, 1), 0)
    device, k = row // 16, row % 16
    second = (k >= 4) & (k < 8)
    fresh_row = (device // 2) * 16 + jnp.where(second, 9, 8)
    own_key = pick(fresh_row, table)
    own_value = pick(fresh_row + KVH * 16, table)
    own = jnp.sum(table.astype(F32) * own_key, axis=1, keepdims=True) * SCALE
    second32 = second[0:32]
    scores = []
    for h in range(KVH):
        rows = table[32 * h : 32 * (h + 1)]
        both = [transposed(rows, cache[r, :, HD * h : HD * (h + 1)]) for r in range(2)]
        scores.append(jnp.where(second32, both[1], both[0]))
    score = jnp.concatenate(scores, axis=0) * SCALE
    alive = iota((256, HD), 1) < jnp.where(second, cache_len[1], cache_len[0])
    weight, own_weight = softmax(score, own, alive)
    values = []
    for h in range(KVH):
        rows = weight[32 * h : 32 * (h + 1)]
        at = HD * (KVH + h)
        both = [
            jnp.dot(rows, cache[r, :, at : at + HD], preferred_element_type=F32)
            for r in range(2)
        ]
        values.append(jnp.where(second32, both[1], both[0]))
    result = jnp.concatenate(values, axis=0) + own_weight * own_value
    arrived = jnp.broadcast_to(landed > 0.5, (256, 1))
    result = jnp.where(arrived & (k == 0), own_key, result)
    result = jnp.where(arrived & (k == 1), own_value, result)
    result = jnp.where(k == 8, terms[0:1, :].astype(F32), result)
    out[...] = result.astype(BF16).reshape(16, 16, HD)


def finish_logprob(masked, received, logprob, values, sems):
    lines = received[:, 8, :].astype(F32)
    take = lambda k: lines[:, 32 * k : 32 * (k + 1)]
    peak, total = take(0), take(1) + take(2) + take(3)
    highest = jnp.max(peak, axis=0, keepdims=True)
    total = jnp.sum(total * jnp.exp(peak - highest), axis=0, keepdims=True)
    normalizer = highest + jnp.log(total)
    row, lane = iota((32, 32), 0), iota((32, 32), 1)
    normalizer = jnp.sum(jnp.where(row == lane, normalizer, 0.0), axis=1, keepdims=True)
    copies = []
    for b in range(4):
        at = slice(BLK * b, BLK * (b + 1))
        section = masked[:, at].astype(F32)
        values[:, at] = jnp.where(section == -jnp.inf, 0.0, section - normalizer)
        copies.append(
            pltpu.make_async_copy(
                values.at[:, pl.ds(BLK * b, BLK)], logprob.at[:, pl.ds(BLK * b, BLK)], sems.at[b]
            )
        )
        copies[-1].start()
    for copy in copies:
        copy.wait()


def attend_landed(mine, other, queries, received, lengths, owners, out):
    turn = lax.axis_index("x")
    prompts = prompts_of(lengths[...], owners[...], lax.axis_index("c8"), turn)
    row = iota((128, 1), 0)
    head, request = row // 32, row % 32
    landed, start, length = landing((request % 2) * 16 + request // 2, prompts)
    even = lax.axis_index("zl") == 0
    keys = jnp.where(even, mine[...], other[...])
    values = jnp.where(even, other[...], mine[...])
    query = jnp.concatenate([queries[:, HD * i : HD * (i + 1)] for i in range(4)], axis=0)
    table = received[...].reshape(256, HD)
    slot = (request // 2) * 16
    own_key = pick(slot, table)
    own_value = pick(slot + 1, table)
    cached = pick(slot + (request % 2) * 4 + head, table)
    own = jnp.sum(query.astype(F32) * own_key, axis=1, keepdims=True) * SCALE
    score = transposed(query, keys) * SCALE
    lane = iota((128, 256), 1)
    position = ((turn + 4 - lane // 64) % 4 * 64 + lane % 64).astype(F32)
    alive = (position >= start) & (position < start + length)
    weight, own_weight = softmax(score, own, alive)
    result = jnp.dot(weight, values, preferred_element_type=F32) + own_weight * own_value
    result = jnp.where(landed > 0.5, result, cached).astype(BF16)
    for i in range(4):
        out[:, HD * i : HD * (i + 1)] = result[32 * i : 32 * (i + 1)]


def exchanged(slots, axis):
    return lax.all_to_all(slots, axis, 0, 0, tiled=True)


def per_device(
    hidden,
    w_kv,
    prompt_lengths,
    owner_step,
    cache,
    cache_len,
    queries,
    fresh,
    logits,
    states,
    masks,
):
    smem = pl.BlockSpec(memory_space=pltpu.SMEM)
    vmem = pl.BlockSpec(memory_space=pltpu.VMEM)
    hbm = pl.BlockSpec(memory_space=pl.ANY)
    sent = jax.ShapeDtypeStruct
    kept = pltpu.VMEM
    held = lambda *values: [
        pltpu.with_memory_space_constraint(value, pltpu.VMEM) for value in values
    ]
    tokens, wide = hidden.shape[0] // 4, hidden.shape[1]
    *shares, asked = pl.pallas_call(
        prepare,
        out_shape=[kept((tokens, wide), BF16)] * 4 + [kept((16, 16, HD), BF16)],
        in_specs=[hbm] * 3,
        out_specs=[vmem] * 5,
        scratch_shapes=[
            pltpu.VMEM(queries.shape, BF16),
            pltpu.VMEM(fresh.shape, BF16),
            pltpu.SemaphoreType.DMA((6,)),
        ],
        name="prepare",
    )(hidden, queries, fresh)
    shares[1:] = [lax.ppermute(shares[k], "x", [(0, k)]) for k in (1, 2, 3)]
    projected = pl.pallas_call(
        project,
        out_shape=sent((16, 80, HD), BF16),
        in_specs=[vmem] * 5 + [hbm],
        scratch_shapes=[pltpu.VMEM(w_kv.shape, BF16), pltpu.SemaphoreType.DMA((4,))],
        name="project",
    )(*held(*shares, asked), w_kv)
    pieces = exchanged(projected, TP)
    masked, terms = pl.pallas_call(
        grammar,
        out_shape=[kept(logits.shape, BF16), kept((16, HD), BF16)],
        in_specs=[vmem] * 3,
        out_specs=[vmem] * 2,
        name="grammar",
    )(*held(logits, states.reshape(1, -1), masks))
    answers = pl.pallas_call(
        attend_cached,
        out_shape=sent((16, 16, HD), BF16),
        in_specs=[smem] + [vmem] * 5,
        name="cached",
    )(cache_len, *held(pieces, cache, terms, prompt_lengths, owner_step))
    answers = exchanged(answers, TP)
    block = pl.pallas_call(
        reduce_blocks,
        out_shape=kept((tokens, HD), BF16),
        in_specs=[vmem],
        out_specs=vmem,
        name="reduce",
    )(*held(pieces))
    around = [
        lax.ppermute(block, "x", [(i, (i + k) % 4) for i in range(4) if (i + k) % 4])
        for k in (1, 2, 3)
    ]
    mine = jnp.concatenate([block] + around, axis=0)
    other = lax.ppermute(mine, "zl", [(0, 1), (1, 0)])
    logprob = pl.pallas_call(
        finish_logprob,
        out_shape=sent(logits.shape, F32),
        in_specs=[vmem] * 2,
        out_specs=hbm,
        scratch_shapes=[pltpu.VMEM(logits.shape, F32), pltpu.SemaphoreType.DMA((4,))],
        name="logprob",
    )(*held(masked, answers))
    attended = pl.pallas_call(
        attend_landed,
        out_shape=sent(queries.shape, BF16),
        in_specs=[vmem] * 6,
        name="landed",
    )(*held(mine, other, queries, answers, prompt_lengths, owner_step))
    return attended, logprob


def solution(mesh):
    groups, columns = mesh.shape["group"], mesh.shape["tp"]
    finer = Mesh(
        mesh.devices.reshape(4, groups // 4, columns // 2, 2), ("x", "c8", "zh", "zl")
    )
    group = ("x", "c8")
    in_specs = (
        P(group, TP),
        P(TP, None),
        P(),
        P(),
        P(group + TP, None, None),
        P(group + TP),
        P(group, TP),
        P(group, TP),
        P(group, TP),
        P(group),
        P(None, TP),
    )
    return jax.shard_map(
        per_device,
        mesh=finer,
        in_specs=in_specs,
        out_specs=(P(group, TP), P(group, TP)),
        check_vma=False,
    )
```

```python
import math

import jax
import jax.numpy as jnp
from jax import lax
from jax.experimental import pallas as pl
from jax.experimental.pallas import tpu as pltpu
from jax.sharding import Mesh, PartitionSpec as P

KVH = 8
HD = 128
STATES = 24
BITS = 30
BLK = 1920
SCALE = 1.0 / math.sqrt(HD)
F32 = jnp.float32
BF16 = jnp.bfloat16
I32 = jnp.int32
TP = ("zh", "zl")


def iota(shape, dim):
    return lax.broadcasted_iota(I32, shape, dim)


def one_hot(target, width):
    rows = target.shape[0]
    return (iota((rows, width), 1) == target).astype(F32).astype(BF16)


def pick(target, table):
    return jnp.dot(one_hot(target, table.shape[0]), table, preferred_element_type=F32)


def prompts_of(lengths, owners, source, turn):
    count = lengths.shape[1]
    here = iota(lengths.shape, 0) == source
    length = jnp.sum(jnp.where(here, lengths, 0).astype(F32), axis=0, keepdims=True)
    owner = jnp.sum(jnp.where(here, owners, 0).astype(F32), axis=0, keepdims=True)
    chosen = ((owner == turn.astype(F32)) & (turn >= 1)).astype(F32)
    row, lane = iota((count, count), 0), iota((count, count), 1)

    def before(values):
        column = jnp.sum(jnp.where(row == lane, values, 0.0), axis=1, keepdims=True)
        return jnp.sum(jnp.where(row < lane, column, 0.0), axis=0, keepdims=True)

    return chosen, before(chosen), before(length), length


def landing(slot, prompts):
    chosen, rank, start, length = prompts
    matched = jnp.where(rank == slot.astype(F32), chosen, 0.0)
    total = lambda values: jnp.sum(matched * values, axis=1, keepdims=True)
    return jnp.sum(matched, axis=1, keepdims=True), total(start), total(length)


def prepare(hidden, queries, fresh, own, first, second, third, asked, query, new, sems):
    shares = [
        pltpu.make_async_copy(hidden.at[pl.ds(64 * k, 64)], out, sems.at[k])
        for k, out in enumerate((own, first, second, third))
    ]
    loads = [
        pltpu.make_async_copy(queries, query, sems.at[4]),
        pltpu.make_async_copy(fresh, new, sems.at[5]),
    ]
    for copy in loads + shares:
        copy.start()
    for copy in loads:
        copy.wait()
    table = jnp.concatenate(
        [query[:, HD * i : HD * (i + 1)] for i in range(4)] + [new[...]], axis=0
    )
    row = iota((256, 1), 0)
    dest, k = row // 16, row % 16
    target = jnp.where(
        k < 8,
        (k % 4) * 32 + 2 * dest + k // 4,
        jnp.where(k < 10, 128 + 2 * dest + k - 8, 160),
    )
    asked[...] = pick(target, table).astype(BF16).reshape(16, 16, HD)
    for copy in shares:
        copy.wait()


def fetch(weight, out, sem):
    copy = pltpu.make_async_copy(weight, out, sem)
    copy.start()
    copy.wait()


def project(own, first, second, third, asked, weight, out):
    turn = lax.axis_index("x")
    tokens = jnp.where(turn == 0, own[...], first[...] + second[...] + third[...])
    full = jnp.dot(tokens, weight[...], preferred_element_type=F32).astype(BF16)
    out[:, 64:80] = asked[...]
    for c in range(16):
        block = c // 2 + (c % 2) * KVH
        out[c, 0:64] = full[:, HD * block : HD * (block + 1)]


def reduce_blocks(pieces, out):
    total = pieces[0, 0:64].astype(F32)
    for c in range(1, 16):
        total = total + pieces[c, 0:64].astype(F32)
    out[...] = total.astype(BF16)


def grammar(logits, states, masks, masked, terms):
    lane = iota((STATES, HD), 1)
    blocks = []
    for half in range(2):
        words = masks[:, HD * half : HD * (half + 1)]
        turned = pltpu.roll(words, 64, 1)
        for x, y in ((words, turned), (turned, words)):
            byte = lambda v, j: jnp.bitwise_and(jnp.right_shift(v, 8 * j), 255)
            blocks.append(
                jnp.concatenate(
                    [
                        jnp.where(lane < 64, byte(x, 0), byte(y, 1)),
                        jnp.where(lane < 64, byte(x, 2), byte(y, 3)),
                    ],
                    axis=1,
                )
            )
    table = jnp.concatenate(blocks, axis=0).astype(F32).astype(BF16)
    row, lane = iota((32, 32), 0), iota((32, 32), 1)
    state = jnp.where(row == lane, states[...], 0).astype(F32)
    state = jnp.sum(state, axis=1, keepdims=True).astype(I32)
    key = jnp.concatenate([state + STATES * b for b in range(4)], axis=0)
    chosen = pick(key, table).astype(BF16)
    column = iota((1, BLK), 1)
    word = jnp.right_shift(column * 34953, 20)
    bit = column - word * BITS
    wanted = jnp.right_shift(bit, 3) * 64 + word
    flag = jnp.left_shift(jnp.ones_like(bit), jnp.bitwise_and(bit, 7))
    spread = (iota((256, BLK), 0) == wanted).astype(F32).astype(BF16)
    peak = None
    kept = []
    for b in range(4):
        value = jnp.dot(
            chosen[32 * b : 32 * (b + 1)], spread, preferred_element_type=F32
        ).astype(I32)
        section = logits[:, BLK * b : BLK * (b + 1)].astype(F32)
        section = jnp.where(jnp.bitwise_and(value, flag) != 0, section, -jnp.inf)
        kept.append(section)
        masked[:, BLK * b : BLK * (b + 1)] = section.astype(BF16)
        top = jnp.max(section, axis=1, keepdims=True)
        peak = top if peak is None else jnp.maximum(peak, top)
    total = sum(jnp.sum(jnp.exp(section - peak), axis=1, keepdims=True) for section in kept)
    high = total.astype(BF16).astype(F32)
    middle = (total - high).astype(BF16).astype(F32)
    low = total - high - middle
    row, lane = iota((32, HD), 0), iota((32, HD), 1)
    spot = lane - row
    line = jnp.where(
        spot == 0, peak, jnp.where(spot == 32, high, jnp.where(spot == 64, middle, low))
    )
    line = jnp.where(jnp.bitwise_and(spot, 31) == 0, line, 0.0)
    terms[...] = jnp.broadcast_to(jnp.sum(line, axis=0, keepdims=True), (16, HD)).astype(BF16)


def softmax(score, own, alive):
    highest = jnp.maximum(
        jnp.max(jnp.where(alive, score, -jnp.inf), axis=1, keepdims=True), own
    )
    exponent = jnp.where(alive, jnp.exp(score - highest), 0.0)
    own_exponent = jnp.exp(own - highest)
    total = jnp.sum(exponent, axis=1, keepdims=True) + own_exponent
    own_weight = (own_exponent / total).astype(BF16).astype(F32)
    return (exponent / total).astype(BF16), own_weight


def transposed(a, b):
    return lax.dot_general(a, b, (((1,), (1,)), ((), ())), preferred_element_type=F32)


def attend_cached(cache_len, received, cache, terms, lengths, owners, out):
    column = lax.axis_index("zh") * 2 + lax.axis_index("zl")
    prompts = prompts_of(
        lengths[...], owners[...], lax.axis_index("c8"), lax.axis_index("x")
    )
    landed = landing(jnp.full((1, 1), column, I32), prompts)[0]
    table = received[:, 64:80, :].reshape(256, HD)
    row = iota((256, 1), 0)
    device, k = row // 16, row % 16
    second = (k >= 4) & (k < 8)
    fresh_row = (device // 2) * 16 + jnp.where(second, 9, 8)
    own_key = pick(fresh_row, table)
    own_value = pick(fresh_row + KVH * 16, table)
    own = jnp.sum(table.astype(F32) * own_key, axis=1, keepdims=True) * SCALE
    second32 = second[0:32]
    scores = []
    for h in range(KVH):
        rows = table[32 * h : 32 * (h + 1)]
        both = [transposed(rows, cache[r, :, HD * h : HD * (h + 1)]) for r in range(2)]
        scores.append(jnp.where(second32, both[1], both[0]))
    score = jnp.concatenate(scores, axis=0) * SCALE
    alive = iota((256, HD), 1) < jnp.where(second, cache_len[1], cache_len[0])
    weight, own_weight = softmax(score, own, alive)
    values = []
    for h in range(KVH):
        rows = weight[32 * h : 32 * (h + 1)]
        at = HD * (KVH + h)
        both = [
            jnp.dot(rows, cache[r, :, at : at + HD], preferred_element_type=F32)
            for r in range(2)
        ]
        values.append(jnp.where(second32, both[1], both[0]))
    result = jnp.concatenate(values, axis=0) + own_weight * own_value
    arrived = jnp.broadcast_to(landed > 0.5, (256, 1))
    result = jnp.where(arrived & (k == 0), own_key, result)
    result = jnp.where(arrived & (k == 1), own_value, result)
    result = jnp.where(k == 8, terms[0:1, :].astype(F32), result)
    out[...] = result.astype(BF16).reshape(16, 16, HD)


def finish_logprob(masked, received, logprob, values, sems):
    lines = received[:, 8, :].astype(F32)
    take = lambda k: lines[:, 32 * k : 32 * (k + 1)]
    peak, total = take(0), take(1) + take(2) + take(3)
    highest = jnp.max(peak, axis=0, keepdims=True)
    total = jnp.sum(total * jnp.exp(peak - highest), axis=0, keepdims=True)
    normalizer = highest + jnp.log(total)
    row, lane = iota((32, 32), 0), iota((32, 32), 1)
    normalizer = jnp.sum(jnp.where(row == lane, normalizer, 0.0), axis=1, keepdims=True)
    copies = []
    for b in range(4):
        at = slice(BLK * b, BLK * (b + 1))
        section = masked[:, at].astype(F32)
        values[:, at] = jnp.where(section == -jnp.inf, 0.0, section - normalizer)
        copies.append(
            pltpu.make_async_copy(
                values.at[:, pl.ds(BLK * b, BLK)], logprob.at[:, pl.ds(BLK * b, BLK)], sems.at[b]
            )
        )
        copies[-1].start()
    for copy in copies:
        copy.wait()


def attend_landed(here, second, first, third, queries, received, lengths, owners, out):
    turn = lax.axis_index("x")
    prompts = prompts_of(lengths[...], owners[...], lax.axis_index("c8"), turn)
    row = iota((128, 1), 0)
    head, request = row // 32, row % 32
    landed, start, length = landing((request % 2) * 16 + request // 2, prompts)
    even = lax.axis_index("zl") == 0
    parts = (here, first, second, third)
    mine = jnp.concatenate([part[0:64] for part in parts], axis=0)
    other = jnp.concatenate([part[64:128] for part in parts], axis=0)
    keys = jnp.where(even, mine, other)
    values = jnp.where(even, other, mine)
    query = jnp.concatenate([queries[:, HD * i : HD * (i + 1)] for i in range(4)], axis=0)
    table = received[...].reshape(256, HD)
    slot = (request // 2) * 16
    own_key = pick(slot, table)
    own_value = pick(slot + 1, table)
    cached = pick(slot + (request % 2) * 4 + head, table)
    own = jnp.sum(query.astype(F32) * own_key, axis=1, keepdims=True) * SCALE
    score = transposed(query, keys) * SCALE
    lane = iota((128, 256), 1)
    position = ((turn + 4 - lane // 64) % 4 * 64 + lane % 64).astype(F32)
    alive = (position >= start) & (position < start + length)
    weight, own_weight = softmax(score, own, alive)
    result = jnp.dot(weight, values, preferred_element_type=F32) + own_weight * own_value
    result = jnp.where(landed > 0.5, result, cached).astype(BF16)
    for i in range(4):
        out[:, HD * i : HD * (i + 1)] = result[32 * i : 32 * (i + 1)]


def exchanged(slots, axis):
    return lax.all_to_all(slots, axis, 0, 0, tiled=True)


def per_device(
    hidden,
    w_kv,
    prompt_lengths,
    owner_step,
    cache,
    cache_len,
    queries,
    fresh,
    logits,
    states,
    masks,
):
    smem = pl.BlockSpec(memory_space=pltpu.SMEM)
    vmem = pl.BlockSpec(memory_space=pltpu.VMEM)
    hbm = pl.BlockSpec(memory_space=pl.ANY)
    sent = jax.ShapeDtypeStruct
    kept = pltpu.VMEM
    held = lambda *values: [
        pltpu.with_memory_space_constraint(value, pltpu.VMEM) for value in values
    ]
    tokens, wide = hidden.shape[0] // 4, hidden.shape[1]
    *shares, asked = pl.pallas_call(
        prepare,
        out_shape=[kept((tokens, wide), BF16)] * 4 + [kept((16, 16, HD), BF16)],
        in_specs=[hbm] * 3,
        out_specs=[vmem] * 5,
        scratch_shapes=[
            pltpu.VMEM(queries.shape, BF16),
            pltpu.VMEM(fresh.shape, BF16),
            pltpu.SemaphoreType.DMA((6,)),
        ],
        name="prepare",
    )(hidden, queries, fresh)
    for k in (2, 1, 3):
        shares[k] = lax.ppermute(shares[k], "x", [(0, k)])
    weight = pl.pallas_call(
        fetch,
        out_shape=kept(w_kv.shape, BF16),
        in_specs=[hbm],
        out_specs=vmem,
        scratch_shapes=[pltpu.SemaphoreType.DMA],
        name="fetch",
    )(w_kv)
    projected = pl.pallas_call(
        project,
        out_shape=sent((16, 80, HD), BF16),
        in_specs=[vmem] * 6,
        name="project",
    )(*held(*shares, asked, weight))
    pieces = exchanged(projected, TP)
    masked, terms = pl.pallas_call(
        grammar,
        out_shape=[kept(logits.shape, BF16), kept((16, HD), BF16)],
        in_specs=[vmem] * 3,
        out_specs=[vmem] * 2,
        name="grammar",
    )(*held(logits, states.reshape(1, -1), masks))
    block = pl.pallas_call(
        reduce_blocks,
        out_shape=kept((tokens, HD), BF16),
        in_specs=[vmem],
        out_specs=vmem,
        name="reduce",
    )(*held(pieces))
    other = lax.ppermute(block, "zl", [(0, 1), (1, 0)])
    answers = pl.pallas_call(
        attend_cached,
        out_shape=sent((16, 16, HD), BF16),
        in_specs=[smem] + [vmem] * 5,
        name="cached",
    )(cache_len, *held(pieces, cache, terms, prompt_lengths, owner_step))
    answers = exchanged(answers, TP)
    both = jnp.concatenate([block, other], axis=0)
    around = [both]
    for k in (2, 1, 3):
        route = [(i, (i + k) % 4) for i in range(4) if (i + k) % 4]
        around.append(lax.ppermute(both, "x", route))
    logprob = pl.pallas_call(
        finish_logprob,
        out_shape=sent(logits.shape, F32),
        in_specs=[vmem] * 2,
        out_specs=hbm,
        scratch_shapes=[pltpu.VMEM(logits.shape, F32), pltpu.SemaphoreType.DMA((4,))],
        name="logprob",
    )(*held(masked, answers))
    attended = pl.pallas_call(
        attend_landed,
        out_shape=sent(queries.shape, BF16),
        in_specs=[vmem] * 8,
        name="landed",
    )(*held(*around, queries, answers, prompt_lengths, owner_step))
    return attended, logprob


def solution(mesh):
    groups, columns = mesh.shape["group"], mesh.shape["tp"]
    finer = Mesh(
        mesh.devices.reshape(4, groups // 4, columns // 2, 2), ("x", "c8", "zh", "zl")
    )
    group = ("x", "c8")
    in_specs = (
        P(group, TP),
        P(TP, None),
        P(),
        P(),
        P(group + TP, None, None),
        P(group + TP),
        P(group, TP),
        P(group, TP),
        P(group, TP),
        P(group),
        P(None, TP),
    )
    return jax.shard_map(
        per_device,
        mesh=finer,
        in_specs=in_specs,
        out_specs=(P(group, TP), P(group, TP)),
        check_vma=False,
    )
```

```python
import math

import jax
import jax.numpy as jnp
from jax import lax
from jax.experimental import pallas as pl
from jax.experimental.pallas import tpu as pltpu
from jax.sharding import Mesh, PartitionSpec as P

KVH = 8
HD = 128
STATES = 24
BITS = 30
BLK = 1920
SCALE = 1.0 / math.sqrt(HD)
F32 = jnp.float32
BF16 = jnp.bfloat16
I32 = jnp.int32
TP = ("zh", "zl")


def iota(shape, dim):
    return lax.broadcasted_iota(I32, shape, dim)


def one_hot(target, width):
    rows = target.shape[0]
    return (iota((rows, width), 1) == target).astype(F32).astype(BF16)


def pick(target, table):
    return jnp.dot(one_hot(target, table.shape[0]), table, preferred_element_type=F32)


def prompts_of(lengths, owners, source, turn):
    count = lengths.shape[1]
    here = iota(lengths.shape, 0) == source
    length = jnp.sum(jnp.where(here, lengths, 0).astype(F32), axis=0, keepdims=True)
    owner = jnp.sum(jnp.where(here, owners, 0).astype(F32), axis=0, keepdims=True)
    chosen = ((owner == turn.astype(F32)) & (turn >= 1)).astype(F32)
    row, lane = iota((count, count), 0), iota((count, count), 1)

    def before(values):
        column = jnp.sum(jnp.where(row == lane, values, 0.0), axis=1, keepdims=True)
        return jnp.sum(jnp.where(row < lane, column, 0.0), axis=0, keepdims=True)

    return chosen, before(chosen), before(length), length


def landing(slot, prompts):
    chosen, rank, start, length = prompts
    matched = jnp.where(rank == slot.astype(F32), chosen, 0.0)
    total = lambda values: jnp.sum(matched * values, axis=1, keepdims=True)
    return jnp.sum(matched, axis=1, keepdims=True), total(start), total(length)


def prepare(hidden, queries, fresh, own, first, second, third, asked, query, new, sems):
    shares = [
        pltpu.make_async_copy(hidden.at[pl.ds(64 * k, 64)], out, sems.at[k])
        for k, out in enumerate((own, first, second, third))
    ]
    loads = [
        pltpu.make_async_copy(queries, query, sems.at[4]),
        pltpu.make_async_copy(fresh, new, sems.at[5]),
    ]
    for copy in loads + shares:
        copy.start()
    for copy in loads:
        copy.wait()
    table = jnp.concatenate(
        [query[:, HD * i : HD * (i + 1)] for i in range(4)] + [new[...]], axis=0
    )
    row = iota((256, 1), 0)
    dest, k = row // 16, row % 16
    target = jnp.where(
        k < 8,
        (k % 4) * 32 + 2 * dest + k // 4,
        jnp.where(k < 10, 128 + 2 * dest + k - 8, 160),
    )
    asked[...] = pick(target, table).astype(BF16).reshape(16, 16, HD)
    for copy in shares:
        copy.wait()


def fetch(weight, out, sem):
    copy = pltpu.make_async_copy(weight, out, sem)
    copy.start()
    copy.wait()


def project(own, first, second, third, weight, out):
    turn = lax.axis_index("x")
    tokens = jnp.where(turn == 0, own[...], first[...] + second[...] + third[...])
    full = jnp.dot(tokens, weight[...], preferred_element_type=F32).astype(BF16)
    for c in range(16):
        block = c // 2 + (c % 2) * KVH
        out[c] = full[:, HD * block : HD * (block + 1)]


def reduce_blocks(pieces, out):
    total = pieces[0].astype(F32)
    for c in range(1, 16):
        total = total + pieces[c].astype(F32)
    out[...] = total.astype(BF16)


def grammar(logits, states, masks, masked, terms):
    lane = iota((STATES, HD), 1)
    blocks = []
    for half in range(2):
        words = masks[:, HD * half : HD * (half + 1)]
        turned = pltpu.roll(words, 64, 1)
        for x, y in ((words, turned), (turned, words)):
            byte = lambda v, j: jnp.bitwise_and(jnp.right_shift(v, 8 * j), 255)
            blocks.append(
                jnp.concatenate(
                    [
                        jnp.where(lane < 64, byte(x, 0), byte(y, 1)),
                        jnp.where(lane < 64, byte(x, 2), byte(y, 3)),
                    ],
                    axis=1,
                )
            )
    table = jnp.concatenate(blocks, axis=0).astype(F32).astype(BF16)
    row, lane = iota((32, 32), 0), iota((32, 32), 1)
    state = jnp.where(row == lane, states[...], 0).astype(F32)
    state = jnp.sum(state, axis=1, keepdims=True).astype(I32)
    key = jnp.concatenate([state + STATES * b for b in range(4)], axis=0)
    chosen = pick(key, table).astype(BF16)
    column = iota((1, BLK), 1)
    word = jnp.right_shift(column * 34953, 20)
    bit = column - word * BITS
    wanted = jnp.right_shift(bit, 3) * 64 + word
    flag = jnp.left_shift(jnp.ones_like(bit), jnp.bitwise_and(bit, 7))
    spread = (iota((256, BLK), 0) == wanted).astype(F32).astype(BF16)
    peak = None
    kept = []
    for b in range(4):
        value = jnp.dot(
            chosen[32 * b : 32 * (b + 1)], spread, preferred_element_type=F32
        ).astype(I32)
        section = logits[:, BLK * b : BLK * (b + 1)].astype(F32)
        section = jnp.where(jnp.bitwise_and(value, flag) != 0, section, -jnp.inf)
        kept.append(section)
        masked[:, BLK * b : BLK * (b + 1)] = section.astype(BF16)
        top = jnp.max(section, axis=1, keepdims=True)
        peak = top if peak is None else jnp.maximum(peak, top)
    total = sum(jnp.sum(jnp.exp(section - peak), axis=1, keepdims=True) for section in kept)
    high = total.astype(BF16).astype(F32)
    middle = (total - high).astype(BF16).astype(F32)
    low = total - high - middle
    row, lane = iota((32, HD), 0), iota((32, HD), 1)
    spot = lane - row
    line = jnp.where(
        spot == 0, peak, jnp.where(spot == 32, high, jnp.where(spot == 64, middle, low))
    )
    line = jnp.where(jnp.bitwise_and(spot, 31) == 0, line, 0.0)
    terms[...] = jnp.broadcast_to(jnp.sum(line, axis=0, keepdims=True), (16, HD)).astype(BF16)


def softmax(score, own, alive):
    highest = jnp.maximum(
        jnp.max(jnp.where(alive, score, -jnp.inf), axis=1, keepdims=True), own
    )
    exponent = jnp.where(alive, jnp.exp(score - highest), 0.0)
    own_exponent = jnp.exp(own - highest)
    total = jnp.sum(exponent, axis=1, keepdims=True) + own_exponent
    own_weight = (own_exponent / total).astype(BF16).astype(F32)
    return (exponent / total).astype(BF16), own_weight


def transposed(a, b):
    return lax.dot_general(a, b, (((1,), (1,)), ((), ())), preferred_element_type=F32)


def attend_cached(cache_len, received, cache, terms, lengths, owners, out):
    column = lax.axis_index("zh") * 2 + lax.axis_index("zl")
    prompts = prompts_of(
        lengths[...], owners[...], lax.axis_index("c8"), lax.axis_index("x")
    )
    landed = landing(jnp.full((1, 1), column, I32), prompts)[0]
    table = received[...].reshape(256, HD)
    row = iota((256, 1), 0)
    device, k = row // 16, row % 16
    second = (k >= 4) & (k < 8)
    fresh_row = (device // 2) * 16 + jnp.where(second, 9, 8)
    own_key = pick(fresh_row, table)
    own_value = pick(fresh_row + KVH * 16, table)
    own = jnp.sum(table.astype(F32) * own_key, axis=1, keepdims=True) * SCALE
    second32 = second[0:32]
    scores = []
    for h in range(KVH):
        rows = table[32 * h : 32 * (h + 1)]
        both = [transposed(rows, cache[r, :, HD * h : HD * (h + 1)]) for r in range(2)]
        scores.append(jnp.where(second32, both[1], both[0]))
    score = jnp.concatenate(scores, axis=0) * SCALE
    alive = iota((256, HD), 1) < jnp.where(second, cache_len[1], cache_len[0])
    weight, own_weight = softmax(score, own, alive)
    values = []
    for h in range(KVH):
        rows = weight[32 * h : 32 * (h + 1)]
        at = HD * (KVH + h)
        both = [
            jnp.dot(rows, cache[r, :, at : at + HD], preferred_element_type=F32)
            for r in range(2)
        ]
        values.append(jnp.where(second32, both[1], both[0]))
    result = jnp.concatenate(values, axis=0) + own_weight * own_value
    arrived = jnp.broadcast_to(landed > 0.5, (256, 1))
    result = jnp.where(arrived & (k == 0), own_key, result)
    result = jnp.where(arrived & (k == 1), own_value, result)
    result = jnp.where(k == 8, terms[0:1, :].astype(F32), result)
    out[...] = result.astype(BF16).reshape(16, 16, HD)


def finish_logprob(masked, received, logprob, values, sems):
    lines = received[:, 8, :].astype(F32)
    take = lambda k: lines[:, 32 * k : 32 * (k + 1)]
    peak, total = take(0), take(1) + take(2) + take(3)
    highest = jnp.max(peak, axis=0, keepdims=True)
    total = jnp.sum(total * jnp.exp(peak - highest), axis=0, keepdims=True)
    normalizer = highest + jnp.log(total)
    row, lane = iota((32, 32), 0), iota((32, 32), 1)
    normalizer = jnp.sum(jnp.where(row == lane, normalizer, 0.0), axis=1, keepdims=True)
    copies = []
    for b in range(4):
        at = slice(BLK * b, BLK * (b + 1))
        section = masked[:, at].astype(F32)
        values[:, at] = jnp.where(section == -jnp.inf, 0.0, section - normalizer)
        copies.append(
            pltpu.make_async_copy(
                values.at[:, pl.ds(BLK * b, BLK)], logprob.at[:, pl.ds(BLK * b, BLK)], sems.at[b]
            )
        )
        copies[-1].start()
    for copy in copies:
        copy.wait()


def attend_landed(here, second, first, third, queries, received, lengths, owners, out):
    turn = lax.axis_index("x")
    prompts = prompts_of(lengths[...], owners[...], lax.axis_index("c8"), turn)
    row = iota((128, 1), 0)
    head, request = row // 32, row % 32
    landed, start, length = landing((request % 2) * 16 + request // 2, prompts)
    even = lax.axis_index("zl") == 0
    parts = (here, first, second, third)
    mine = jnp.concatenate([part[0:64] for part in parts], axis=0)
    other = jnp.concatenate([part[64:128] for part in parts], axis=0)
    keys = jnp.where(even, mine, other)
    values = jnp.where(even, other, mine)
    query = jnp.concatenate([queries[:, HD * i : HD * (i + 1)] for i in range(4)], axis=0)
    table = received[...].reshape(256, HD)
    slot = (request // 2) * 16
    own_key = pick(slot, table)
    own_value = pick(slot + 1, table)
    cached = pick(slot + (request % 2) * 4 + head, table)
    own = jnp.sum(query.astype(F32) * own_key, axis=1, keepdims=True) * SCALE
    score = transposed(query, keys) * SCALE
    lane = iota((128, 256), 1)
    position = ((turn + 4 - lane // 64) % 4 * 64 + lane % 64).astype(F32)
    alive = (position >= start) & (position < start + length)
    weight, own_weight = softmax(score, own, alive)
    result = jnp.dot(weight, values, preferred_element_type=F32) + own_weight * own_value
    result = jnp.where(landed > 0.5, result, cached).astype(BF16)
    for i in range(4):
        out[:, HD * i : HD * (i + 1)] = result[32 * i : 32 * (i + 1)]


def exchanged(slots, axis):
    return lax.all_to_all(slots, axis, 0, 0, tiled=True)


def per_device(
    hidden,
    w_kv,
    prompt_lengths,
    owner_step,
    cache,
    cache_len,
    queries,
    fresh,
    logits,
    states,
    masks,
):
    smem = pl.BlockSpec(memory_space=pltpu.SMEM)
    vmem = pl.BlockSpec(memory_space=pltpu.VMEM)
    hbm = pl.BlockSpec(memory_space=pl.ANY)
    sent = jax.ShapeDtypeStruct
    kept = pltpu.VMEM
    held = lambda *values: [
        pltpu.with_memory_space_constraint(value, pltpu.VMEM) for value in values
    ]
    tokens, wide = hidden.shape[0] // 4, hidden.shape[1]
    *shares, asked = pl.pallas_call(
        prepare,
        out_shape=[kept((tokens, wide), BF16)] * 4 + [sent((16, 16, HD), BF16)],
        in_specs=[hbm] * 3,
        out_specs=[vmem] * 5,
        scratch_shapes=[
            pltpu.VMEM(queries.shape, BF16),
            pltpu.VMEM(fresh.shape, BF16),
            pltpu.SemaphoreType.DMA((6,)),
        ],
        name="prepare",
    )(hidden, queries, fresh)
    for k in (2, 1, 3):
        shares[k] = lax.ppermute(shares[k], "x", [(0, k)])
    asked = exchanged(asked, TP)
    weight = pl.pallas_call(
        fetch,
        out_shape=kept(w_kv.shape, BF16),
        in_specs=[hbm],
        out_specs=vmem,
        scratch_shapes=[pltpu.SemaphoreType.DMA],
        name="fetch",
    )(w_kv)
    projected = pl.pallas_call(
        project,
        out_shape=sent((16, tokens, HD), BF16),
        in_specs=[vmem] * 5,
        name="project",
    )(*held(*shares, weight))
    pieces = exchanged(projected, TP)
    masked, terms = pl.pallas_call(
        grammar,
        out_shape=[kept(logits.shape, BF16), kept((16, HD), BF16)],
        in_specs=[vmem] * 3,
        out_specs=[vmem] * 2,
        name="grammar",
    )(*held(logits, states.reshape(1, -1), masks))
    block = pl.pallas_call(
        reduce_blocks,
        out_shape=kept((tokens, HD), BF16),
        in_specs=[vmem],
        out_specs=vmem,
        name="reduce",
    )(*held(pieces))
    other = lax.ppermute(block, "zl", [(0, 1), (1, 0)])
    answers = pl.pallas_call(
        attend_cached,
        out_shape=sent((16, 16, HD), BF16),
        in_specs=[smem] + [vmem] * 5,
        name="cached",
    )(cache_len, *held(asked, cache, terms, prompt_lengths, owner_step))
    answers = exchanged(answers, TP)
    both = jnp.concatenate([block, other], axis=0)
    around = [both]
    for k in (2, 1, 3):
        route = [(i, (i + k) % 4) for i in range(4) if (i + k) % 4]
        around.append(lax.ppermute(both, "x", route))
    logprob = pl.pallas_call(
        finish_logprob,
        out_shape=sent(logits.shape, F32),
        in_specs=[vmem] * 2,
        out_specs=hbm,
        scratch_shapes=[pltpu.VMEM(logits.shape, F32), pltpu.SemaphoreType.DMA((4,))],
        name="logprob",
    )(*held(masked, answers))
    attended = pl.pallas_call(
        attend_landed,
        out_shape=sent(queries.shape, BF16),
        in_specs=[vmem] * 8,
        name="landed",
    )(*held(*around, queries, answers, prompt_lengths, owner_step))
    return attended, logprob


def solution(mesh):
    groups, columns = mesh.shape["group"], mesh.shape["tp"]
    finer = Mesh(
        mesh.devices.reshape(4, groups // 4, columns // 2, 2), ("x", "c8", "zh", "zl")
    )
    group = ("x", "c8")
    in_specs = (
        P(group, TP),
        P(TP, None),
        P(),
        P(),
        P(group + TP, None, None),
        P(group + TP),
        P(group, TP),
        P(group, TP),
        P(group, TP),
        P(group),
        P(None, TP),
    )
    return jax.shard_map(
        per_device,
        mesh=finer,
        in_specs=in_specs,
        out_specs=(P(group, TP), P(group, TP)),
        check_vma=False,
    )
```

```python
import math

import jax
import jax.numpy as jnp
from jax import lax
from jax.experimental import pallas as pl
from jax.experimental.pallas import tpu as pltpu
from jax.sharding import Mesh, PartitionSpec as P

KVH = 8
HD = 128
STATES = 24
BITS = 30
LOWEST = -1e30
BLK = 1920
SCALE = 1.0 / math.sqrt(HD)
F32 = jnp.float32
BF16 = jnp.bfloat16
I32 = jnp.int32
TP = ("zh", "zl")


def iota(shape, dim):
    return lax.broadcasted_iota(I32, shape, dim)


def one_hot(target, width):
    rows = target.shape[0]
    return (iota((rows, width), 1) == target).astype(F32).astype(BF16)


def pick(target, table):
    return jnp.dot(one_hot(target, table.shape[0]), table, preferred_element_type=F32)


def prompts_of(lengths, owners, source, turn):
    count = lengths.shape[1]
    here = iota(lengths.shape, 0) == source
    length = jnp.sum(jnp.where(here, lengths, 0).astype(F32), axis=0, keepdims=True)
    owner = jnp.sum(jnp.where(here, owners, 0).astype(F32), axis=0, keepdims=True)
    chosen = ((owner == turn.astype(F32)) & (turn >= 1)).astype(F32)
    row, lane = iota((count, count), 0), iota((count, count), 1)

    def before(values):
        column = jnp.sum(jnp.where(row == lane, values, 0.0), axis=1, keepdims=True)
        return jnp.sum(jnp.where(row < lane, column, 0.0), axis=0, keepdims=True)

    return chosen, before(chosen), before(length), length


def landing(slot, prompts):
    chosen, rank, start, length = prompts
    matched = jnp.where(rank == slot.astype(F32), chosen, 0.0)
    total = lambda values: jnp.sum(matched * values, axis=1, keepdims=True)
    return jnp.sum(matched, axis=1, keepdims=True), total(start), total(length)


def prepare(hidden, queries, fresh, own, first, second, third, asked, query, new, sems):
    shares = [
        pltpu.make_async_copy(hidden.at[pl.ds(64 * k, 64)], out, sems.at[k])
        for k, out in enumerate((own, first, second, third))
    ]
    loads = [
        pltpu.make_async_copy(queries, query, sems.at[4]),
        pltpu.make_async_copy(fresh, new, sems.at[5]),
    ]
    for copy in loads + shares:
        copy.start()
    for copy in loads:
        copy.wait()
    table = jnp.concatenate(
        [query[:, HD * i : HD * (i + 1)] for i in range(4)] + [new[...]], axis=0
    )
    row = iota((256, 1), 0)
    dest, k = row // 16, row % 16
    target = jnp.where(
        k < 8,
        (k % 4) * 32 + 2 * dest + k // 4,
        jnp.where(k < 10, 128 + 2 * dest + k - 8, 160),
    )
    asked[...] = pick(target, table).astype(BF16).reshape(16, 16, HD)
    for copy in shares:
        copy.wait()


def fetch(weight, out, sem):
    copy = pltpu.make_async_copy(weight, out, sem)
    copy.start()
    copy.wait()


def project(own, first, second, third, asked, weight, out, slots, sems):
    turn = lax.axis_index("x")
    tokens = jnp.where(turn == 0, own[...], first[...] + second[...] + third[...])
    slots[:, 64:80] = asked[...]
    copies = []
    for h in range(4):
        for part in range(2):
            at = HD * (KVH * part + 2 * h)
            full = jnp.dot(
                tokens, weight[:, at : at + 2 * HD], preferred_element_type=F32
            ).astype(BF16)
            slots[4 * h + part, 0:64] = full[:, :HD]
            slots[4 * h + 2 + part, 0:64] = full[:, HD:]
        four = pl.ds(4 * h, 4)
        copies.append(pltpu.make_async_copy(slots.at[four], out.at[four], sems.at[h]))
        copies[-1].start()
    for copy in copies:
        copy.wait()


def reduce_blocks(pieces, out):
    total = pieces[0, 0:64].astype(F32)
    for c in range(1, 16):
        total = total + pieces[c, 0:64].astype(F32)
    out[...] = total.astype(BF16)


def grammar(logits, states, masks, masked, terms):
    lane = iota((STATES, HD), 1)
    blocks = []
    for half in range(2):
        words = masks[:, HD * half : HD * (half + 1)]
        turned = pltpu.roll(words, 64, 1)
        for x, y in ((words, turned), (turned, words)):
            byte = lambda v, j: jnp.bitwise_and(jnp.right_shift(v, 8 * j), 255)
            blocks.append(
                jnp.concatenate(
                    [
                        jnp.where(lane < 64, byte(x, 0), byte(y, 1)),
                        jnp.where(lane < 64, byte(x, 2), byte(y, 3)),
                    ],
                    axis=1,
                )
            )
    table = jnp.concatenate(blocks, axis=0).astype(F32).astype(BF16)
    row, lane = iota((32, 32), 0), iota((32, 32), 1)
    state = jnp.where(row == lane, states[...], 0).astype(F32)
    state = jnp.sum(state, axis=1, keepdims=True).astype(I32)
    key = jnp.concatenate([state + STATES * b for b in range(4)], axis=0)
    chosen = pick(key, table).astype(BF16)
    column = iota((1, BLK), 1)
    word = jnp.right_shift(column * 34953, 20)
    bit = column - word * BITS
    wanted = jnp.right_shift(bit, 3) * 64 + word
    flag = jnp.left_shift(jnp.ones_like(bit), jnp.bitwise_and(bit, 7))
    spread = (iota((256, BLK), 0) == wanted).astype(F32).astype(BF16)
    peak = None
    kept = []
    for b in range(4):
        value = jnp.dot(
            chosen[32 * b : 32 * (b + 1)], spread, preferred_element_type=F32
        ).astype(I32)
        section = logits[:, BLK * b : BLK * (b + 1)].astype(F32)
        section = jnp.where(jnp.bitwise_and(value, flag) != 0, section, -jnp.inf)
        kept.append(section)
        masked[:, BLK * b : BLK * (b + 1)] = section.astype(BF16)
        top = jnp.max(section, axis=1, keepdims=True)
        peak = top if peak is None else jnp.maximum(peak, top)
    total = sum(jnp.sum(jnp.exp(section - peak), axis=1, keepdims=True) for section in kept)
    high = total.astype(BF16).astype(F32)
    middle = (total - high).astype(BF16).astype(F32)
    low = total - high - middle
    row, lane = iota((32, HD), 0), iota((32, HD), 1)
    spot = lane - row
    line = jnp.where(
        spot == 0, peak, jnp.where(spot == 32, high, jnp.where(spot == 64, middle, low))
    )
    line = jnp.where(jnp.bitwise_and(spot, 31) == 0, line, 0.0)
    terms[...] = jnp.broadcast_to(jnp.sum(line, axis=0, keepdims=True), (16, HD)).astype(BF16)


def softmax(score, own, alive):
    highest = jnp.maximum(
        jnp.max(jnp.where(alive, score, -jnp.inf), axis=1, keepdims=True), own
    )
    exponent = jnp.where(alive, jnp.exp(score - highest), 0.0)
    own_exponent = jnp.exp(own - highest)
    total = jnp.sum(exponent, axis=1, keepdims=True) + own_exponent
    own_weight = (own_exponent / total).astype(BF16).astype(F32)
    return (exponent / total).astype(BF16), own_weight


def transposed(a, b):
    return lax.dot_general(a, b, (((1,), (1,)), ((), ())), preferred_element_type=F32)


def attend_cached(cache_len, received, cache, terms, lengths, owners, out):
    column = lax.axis_index("zh") * 2 + lax.axis_index("zl")
    prompts = prompts_of(
        lengths[...], owners[...], lax.axis_index("c8"), lax.axis_index("x")
    )
    landed = landing(jnp.full((1, 1), column, I32), prompts)[0]
    table = received[:, 64:80, :].reshape(256, HD)
    row = iota((256, 1), 0)
    device, k = row // 16, row % 16
    second = (k >= 4) & (k < 8)
    fresh_row = (device // 2) * 16 + jnp.where(second, 9, 8)
    own_key = pick(fresh_row, table)
    own_value = pick(fresh_row + KVH * 16, table)
    own = jnp.sum(table.astype(F32) * own_key, axis=1, keepdims=True) * SCALE
    second32 = second[0:32]
    scores = []
    for h in range(KVH):
        rows = table[32 * h : 32 * (h + 1)]
        both = [transposed(rows, cache[r, :, HD * h : HD * (h + 1)]) for r in range(2)]
        scores.append(jnp.where(second32, both[1], both[0]))
    score = jnp.concatenate(scores, axis=0) * SCALE
    alive = iota((256, HD), 1) < jnp.where(second, cache_len[0:1, 1:2], cache_len[0:1, 0:1])
    weight, own_weight = softmax(score, own, alive)
    values = []
    for h in range(KVH):
        rows = weight[32 * h : 32 * (h + 1)]
        at = HD * (KVH + h)
        both = [
            jnp.dot(rows, cache[r, :, at : at + HD], preferred_element_type=F32)
            for r in range(2)
        ]
        values.append(jnp.where(second32, both[1], both[0]))
    result = jnp.concatenate(values, axis=0) + own_weight * own_value
    arrived = jnp.broadcast_to(landed > 0.5, (256, 1))
    result = jnp.where(arrived & (k == 0), own_key, result)
    result = jnp.where(arrived & (k == 1), own_value, result)
    result = jnp.where(k == 8, terms[0:1, :].astype(F32), result)
    out[...] = result.astype(BF16).reshape(16, 16, HD)


def attend_prompts(here, second, first, third, queries, lengths, owners, result, stats):
    turn = lax.axis_index("x")
    prompts = prompts_of(lengths[...], owners[...], lax.axis_index("c8"), turn)
    request = iota((128, 1), 0) % 32
    landed, start, length = landing((request % 2) * 16 + request // 2, prompts)
    even = lax.axis_index("zl") == 0
    parts = (here, first, second, third)
    mine = jnp.concatenate([part[0:64] for part in parts], axis=0)
    other = jnp.concatenate([part[64:128] for part in parts], axis=0)
    keys = jnp.where(even, mine, other)
    values = jnp.where(even, other, mine)
    query = jnp.concatenate([queries[:, HD * i : HD * (i + 1)] for i in range(4)], axis=0)
    score = transposed(query, keys) * SCALE
    lane = iota((128, 256), 1)
    position = ((turn + 4 - lane // 64) % 4 * 64 + lane % 64).astype(F32)
    alive = (position >= start) & (position < start + length)
    highest = jnp.max(jnp.where(alive, score, LOWEST), axis=1, keepdims=True)
    exponent = jnp.where(alive, jnp.exp(score - highest), 0.0)
    result[...] = jnp.dot(exponent.astype(BF16), values, preferred_element_type=F32)
    total = jnp.sum(exponent, axis=1, keepdims=True)
    lane = iota((128, HD), 1)
    stats[...] = jnp.where(lane == 0, highest, jnp.where(lane == 1, total, landed))


def finish(masked, received, queries, result, stats, logprob, attended, values, sems):
    lines = received[:, 8, :].astype(F32)
    take = lambda k: lines[:, 32 * k : 32 * (k + 1)]
    peak, total = take(0), take(1) + take(2) + take(3)
    highest = jnp.max(peak, axis=0, keepdims=True)
    total = jnp.sum(total * jnp.exp(peak - highest), axis=0, keepdims=True)
    normalizer = highest + jnp.log(total)
    row, lane = iota((32, 32), 0), iota((32, 32), 1)
    normalizer = jnp.sum(jnp.where(row == lane, normalizer, 0.0), axis=1, keepdims=True)
    copies = []
    for b in range(4):
        at = slice(BLK * b, BLK * (b + 1))
        section = masked[:, at].astype(F32)
        values[:, at] = jnp.where(section == -jnp.inf, 0.0, section - normalizer)
        piece = pl.ds(BLK * b, BLK)
        copies.append(
            pltpu.make_async_copy(values.at[:, piece], logprob.at[:, piece], sems.at[b])
        )
        copies[-1].start()
    row = iota((128, 1), 0)
    head, request = row // 32, row % 32
    query = jnp.concatenate([queries[:, HD * i : HD * (i + 1)] for i in range(4)], axis=0)
    table = received[...].reshape(256, HD)
    slot = (request // 2) * 16
    target = jnp.concatenate([slot, slot + 1, slot + (request % 2) * 4 + head], axis=0)
    picked = pick(target, table)
    own_key, own_value, cached = picked[0:128], picked[128:256], picked[256:384]
    own = jnp.sum(query.astype(F32) * own_key, axis=1, keepdims=True) * SCALE
    top, total, landed = stats[:, 0:1], stats[:, 1:2], stats[:, 2:3]
    highest = jnp.maximum(top, own)
    share, own_share = jnp.exp(top - highest), jnp.exp(own - highest)
    scale = 1.0 / (total * share + own_share)
    merged = (result[...] * share + own_value * own_share) * scale
    merged = jnp.where(landed > 0.5, merged, cached).astype(BF16)
    for i in range(4):
        attended[:, HD * i : HD * (i + 1)] = merged[32 * i : 32 * (i + 1)]
    for copy in copies:
        copy.wait()


def exchanged(slots, axis):
    return lax.all_to_all(slots, axis, 0, 0, tiled=True)


def per_device(
    hidden,
    w_kv,
    prompt_lengths,
    owner_step,
    cache,
    cache_len,
    queries,
    fresh,
    logits,
    states,
    masks,
):
    vmem = pl.BlockSpec(memory_space=pltpu.VMEM)
    hbm = pl.BlockSpec(memory_space=pl.ANY)
    sent = jax.ShapeDtypeStruct
    kept = pltpu.VMEM
    held = lambda *values: [
        pltpu.with_memory_space_constraint(value, pltpu.VMEM) for value in values
    ]
    tokens, wide = hidden.shape[0] // 4, hidden.shape[1]
    *shares, asked = pl.pallas_call(
        prepare,
        out_shape=[kept((tokens, wide), BF16)] * 4 + [kept((16, 16, HD), BF16)],
        in_specs=[hbm] * 3,
        out_specs=[vmem] * 5,
        scratch_shapes=[
            pltpu.VMEM(queries.shape, BF16),
            pltpu.VMEM(fresh.shape, BF16),
            pltpu.SemaphoreType.DMA((6,)),
        ],
        name="prepare",
    )(hidden, queries, fresh)
    for k in (2, 1, 3):
        shares[k] = lax.ppermute(shares[k], "x", [(0, k)])
    weight = pl.pallas_call(
        fetch,
        out_shape=kept(w_kv.shape, BF16),
        in_specs=[hbm],
        out_specs=vmem,
        scratch_shapes=[pltpu.SemaphoreType.DMA],
        name="fetch",
    )(w_kv)
    projected = pl.pallas_call(
        project,
        out_shape=sent((16, 80, HD), BF16),
        in_specs=[vmem] * 6,
        out_specs=hbm,
        scratch_shapes=[pltpu.VMEM((16, 80, HD), BF16), pltpu.SemaphoreType.DMA((4,))],
        name="project",
    )(*held(*shares, asked, weight))
    pieces = exchanged(projected, TP)
    masked, terms = pl.pallas_call(
        grammar,
        out_shape=[kept(logits.shape, BF16), kept((16, HD), BF16)],
        in_specs=[vmem] * 3,
        out_specs=[vmem] * 2,
        name="grammar",
    )(*held(logits, states.reshape(1, -1), masks))
    block = pl.pallas_call(
        reduce_blocks,
        out_shape=kept((tokens, HD), BF16),
        in_specs=[vmem],
        out_specs=vmem,
        name="reduce",
    )(*held(pieces))
    other = lax.ppermute(block, "zl", [(0, 1), (1, 0)])
    answers = pl.pallas_call(
        attend_cached,
        out_shape=sent((16, 16, HD), BF16),
        in_specs=[vmem] * 6,
        name="cached",
    )(*held(cache_len.reshape(1, 2), pieces, cache, terms, prompt_lengths, owner_step))
    answers = exchanged(answers, TP)
    both = jnp.concatenate([block, other], axis=0)
    around = [both]
    for k in (2, 1, 3):
        route = [(i, (i + k) % 4) for i in range(4) if (i + k) % 4]
        around.append(lax.ppermute(both, "x", route))
    result, stats = pl.pallas_call(
        attend_prompts,
        out_shape=[kept((128, HD), F32), kept((128, HD), F32)],
        in_specs=[vmem] * 7,
        out_specs=[vmem] * 2,
        name="prompts",
    )(*held(*around, queries, prompt_lengths, owner_step))
    logprob, attended = pl.pallas_call(
        finish,
        out_shape=[sent(logits.shape, F32), sent(queries.shape, BF16)],
        in_specs=[vmem] * 5,
        out_specs=[hbm, vmem],
        scratch_shapes=[pltpu.VMEM(logits.shape, F32), pltpu.SemaphoreType.DMA((4,))],
        name="finish",
    )(*held(masked, answers, queries, result, stats))
    return attended, logprob


def solution(mesh):
    groups, columns = mesh.shape["group"], mesh.shape["tp"]
    finer = Mesh(
        mesh.devices.reshape(4, groups // 4, columns // 2, 2), ("x", "c8", "zh", "zl")
    )
    group = ("x", "c8")
    in_specs = (
        P(group, TP),
        P(TP, None),
        P(),
        P(),
        P(group + TP, None, None),
        P(group + TP),
        P(group, TP),
        P(group, TP),
        P(group, TP),
        P(group),
        P(None, TP),
    )
    return jax.shard_map(
        per_device,
        mesh=finer,
        in_specs=in_specs,
        out_specs=(P(group, TP), P(group, TP)),
        check_vma=False,
    )
```

```python
import math

import jax
import jax.numpy as jnp
from jax import lax
from jax.experimental import pallas as pl
from jax.experimental.pallas import tpu as pltpu
from jax.sharding import Mesh, PartitionSpec as P

KVH = 8
HD = 128
STATES = 24
BITS = 30
LOWEST = -1e30
BLK = 1920
SCALE = 1.0 / math.sqrt(HD)
F32 = jnp.float32
BF16 = jnp.bfloat16
I32 = jnp.int32
TP = ("zh", "zl")


def iota(shape, dim):
    return lax.broadcasted_iota(I32, shape, dim)


def one_hot(target, width):
    rows = target.shape[0]
    return (iota((rows, width), 1) == target).astype(F32).astype(BF16)


def pick(target, table):
    return jnp.dot(one_hot(target, table.shape[0]), table, preferred_element_type=F32)


def prompts_of(lengths, owners, source, turn):
    count = lengths.shape[1]
    here = iota(lengths.shape, 0) == source
    length = jnp.sum(jnp.where(here, lengths, 0).astype(F32), axis=0, keepdims=True)
    owner = jnp.sum(jnp.where(here, owners, 0).astype(F32), axis=0, keepdims=True)
    chosen = ((owner == turn.astype(F32)) & (turn >= 1)).astype(F32)
    row, lane = iota((count, count), 0), iota((count, count), 1)

    def before(values):
        column = jnp.sum(jnp.where(row == lane, values, 0.0), axis=1, keepdims=True)
        return jnp.sum(jnp.where(row < lane, column, 0.0), axis=0, keepdims=True)

    return chosen, before(chosen), before(length), length


def landing(slot, prompts):
    chosen, rank, start, length = prompts
    matched = jnp.where(rank == slot.astype(F32), chosen, 0.0)
    total = lambda values: jnp.sum(matched * values, axis=1, keepdims=True)
    return jnp.sum(matched, axis=1, keepdims=True), total(start), total(length)


def prepare(hidden, queries, fresh, own, first, second, third, asked, query, new, sems):
    shares = [
        pltpu.make_async_copy(hidden.at[pl.ds(64 * k, 64)], out, sems.at[k])
        for k, out in enumerate((own, first, second, third))
    ]
    loads = [
        pltpu.make_async_copy(queries, query, sems.at[4]),
        pltpu.make_async_copy(fresh, new, sems.at[5]),
    ]
    for copy in loads + shares:
        copy.start()
    for copy in loads:
        copy.wait()
    table = jnp.concatenate(
        [query[:, HD * i : HD * (i + 1)] for i in range(4)] + [new[...]], axis=0
    )
    row = iota((256, 1), 0)
    dest, k = row // 16, row % 16
    target = jnp.where(
        k < 8,
        (k % 4) * 32 + 2 * dest + k // 4,
        jnp.where(k < 10, 128 + 2 * dest + k - 8, 160),
    )
    asked[...] = pick(target, table).astype(BF16).reshape(16, 16, HD)
    for copy in shares:
        copy.wait()


def fetch(weight, out, sem):
    copy = pltpu.make_async_copy(weight, out, sem)
    copy.start()
    copy.wait()


def project(own, first, second, third, asked, weight, out, slots, sems):
    turn = lax.axis_index("x")
    tokens = jnp.where(turn == 0, own[...], first[...] + second[...] + third[...])
    slots[:, 64:80] = asked[...]
    copies = []
    for h in range(4):
        for part in range(2):
            at = HD * (KVH * part + 2 * h)
            full = jnp.dot(
                tokens, weight[:, at : at + 2 * HD], preferred_element_type=F32
            ).astype(BF16)
            slots[4 * h + part, 0:64] = full[:, :HD]
            slots[4 * h + 2 + part, 0:64] = full[:, HD:]
        four = pl.ds(4 * h, 4)
        copies.append(pltpu.make_async_copy(slots.at[four], out.at[four], sems.at[h]))
        copies[-1].start()
    for copy in copies:
        copy.wait()


def reduce_blocks(pieces, out):
    total = pieces[0, 0:64].astype(F32)
    for c in range(1, 16):
        total = total + pieces[c, 0:64].astype(F32)
    out[...] = total.astype(BF16)


def grammar(logits, states, masks, masked, terms):
    lane = iota((STATES, HD), 1)
    blocks = []
    for half in range(2):
        words = masks[:, HD * half : HD * (half + 1)]
        turned = pltpu.roll(words, 64, 1)
        for x, y in ((words, turned), (turned, words)):
            byte = lambda v, j: jnp.bitwise_and(jnp.right_shift(v, 8 * j), 255)
            blocks.append(
                jnp.concatenate(
                    [
                        jnp.where(lane < 64, byte(x, 0), byte(y, 1)),
                        jnp.where(lane < 64, byte(x, 2), byte(y, 3)),
                    ],
                    axis=1,
                )
            )
    table = jnp.concatenate(blocks, axis=0).astype(F32).astype(BF16)
    row, lane = iota((32, 32), 0), iota((32, 32), 1)
    state = jnp.where(row == lane, states[...], 0).astype(F32)
    state = jnp.sum(state, axis=1, keepdims=True).astype(I32)
    key = jnp.concatenate([state + STATES * b for b in range(4)], axis=0)
    chosen = pick(key, table).astype(BF16)
    column = iota((1, BLK), 1)
    word = jnp.right_shift(column * 34953, 20)
    bit = column - word * BITS
    wanted = jnp.right_shift(bit, 3) * 64 + word
    flag = jnp.left_shift(jnp.ones_like(bit), jnp.bitwise_and(bit, 7))
    spread = (iota((256, BLK), 0) == wanted).astype(F32).astype(BF16)
    peak = None
    kept = []
    for b in range(4):
        value = jnp.dot(
            chosen[32 * b : 32 * (b + 1)], spread, preferred_element_type=F32
        ).astype(I32)
        section = logits[:, BLK * b : BLK * (b + 1)].astype(F32)
        section = jnp.where(jnp.bitwise_and(value, flag) != 0, section, -jnp.inf)
        kept.append(section)
        masked[:, BLK * b : BLK * (b + 1)] = section.astype(BF16)
        top = jnp.max(section, axis=1, keepdims=True)
        peak = top if peak is None else jnp.maximum(peak, top)
    total = sum(jnp.sum(jnp.exp(section - peak), axis=1, keepdims=True) for section in kept)
    high = total.astype(BF16).astype(F32)
    middle = (total - high).astype(BF16).astype(F32)
    low = total - high - middle
    row, lane = iota((32, HD), 0), iota((32, HD), 1)
    spot = lane - row
    line = jnp.where(
        spot == 0, peak, jnp.where(spot == 32, high, jnp.where(spot == 64, middle, low))
    )
    line = jnp.where(jnp.bitwise_and(spot, 31) == 0, line, 0.0)
    terms[...] = jnp.broadcast_to(jnp.sum(line, axis=0, keepdims=True), (16, HD)).astype(BF16)


def softmax(score, own, alive):
    highest = jnp.maximum(
        jnp.max(jnp.where(alive, score, -jnp.inf), axis=1, keepdims=True), own
    )
    exponent = jnp.where(alive, jnp.exp(score - highest), 0.0)
    own_exponent = jnp.exp(own - highest)
    total = jnp.sum(exponent, axis=1, keepdims=True) + own_exponent
    own_weight = (own_exponent / total).astype(BF16).astype(F32)
    return (exponent / total).astype(BF16), own_weight


def transposed(a, b):
    return lax.dot_general(a, b, (((1,), (1,)), ((), ())), preferred_element_type=F32)


def attend_cached(cache_len, received, cache, terms, lengths, owners, out):
    column = lax.axis_index("zh") * 2 + lax.axis_index("zl")
    prompts = prompts_of(
        lengths[...], owners[...], lax.axis_index("c8"), lax.axis_index("x")
    )
    landed = landing(jnp.full((1, 1), column, I32), prompts)[0]
    table = received[:, 64:80, :].reshape(256, HD)
    row = iota((256, 1), 0)
    device, k = row // 16, row % 16
    second = (k >= 4) & (k < 8)
    fresh_row = (device // 2) * 16 + jnp.where(second, 9, 8)
    own_key = pick(fresh_row, table)
    own_value = pick(fresh_row + KVH * 16, table)
    own = jnp.sum(table.astype(F32) * own_key, axis=1, keepdims=True) * SCALE
    second32 = second[0:32]
    scores = []
    for h in range(KVH):
        rows = table[32 * h : 32 * (h + 1)]
        both = [transposed(rows, cache[r, :, HD * h : HD * (h + 1)]) for r in range(2)]
        scores.append(jnp.where(second32, both[1], both[0]))
    score = jnp.concatenate(scores, axis=0) * SCALE
    alive = iota((256, HD), 1) < jnp.where(second, cache_len[0:1, 1:2], cache_len[0:1, 0:1])
    weight, own_weight = softmax(score, own, alive)
    values = []
    for h in range(KVH):
        rows = weight[32 * h : 32 * (h + 1)]
        at = HD * (KVH + h)
        both = [
            jnp.dot(rows, cache[r, :, at : at + HD], preferred_element_type=F32)
            for r in range(2)
        ]
        values.append(jnp.where(second32, both[1], both[0]))
    result = jnp.concatenate(values, axis=0) + own_weight * own_value
    arrived = jnp.broadcast_to(landed > 0.5, (256, 1))
    result = jnp.where(arrived & (k == 0), own_key, result)
    result = jnp.where(arrived & (k == 1), own_value, result)
    result = jnp.where(k == 8, terms[0:1, :].astype(F32), result)
    out[...] = result.astype(BF16).reshape(16, 16, HD)


def attend_prompts(parts, queries, lengths, owners, result, stats):
    prompts = prompts_of(
        lengths[...], owners[...], lax.axis_index("c8"), lax.axis_index("x")
    )
    request = iota((128, 1), 0) % 32
    landed, start, length = landing((request % 2) * 16 + request // 2, prompts)
    even = lax.axis_index("zl") == 0
    mine = jnp.concatenate([parts[x, 0:64] for x in range(4)], axis=0)
    other = jnp.concatenate([parts[x, 64:128] for x in range(4)], axis=0)
    keys = jnp.where(even, mine, other)
    values = jnp.where(even, other, mine)
    query = jnp.concatenate([queries[:, HD * i : HD * (i + 1)] for i in range(4)], axis=0)
    score = transposed(query, keys) * SCALE
    position = iota((128, 256), 1).astype(F32)
    alive = (position >= start) & (position < start + length)
    highest = jnp.max(jnp.where(alive, score, LOWEST), axis=1, keepdims=True)
    exponent = jnp.where(alive, jnp.exp(score - highest), 0.0)
    result[...] = jnp.dot(exponent.astype(BF16), values, preferred_element_type=F32)
    total = jnp.sum(exponent, axis=1, keepdims=True)
    lane = iota((128, HD), 1)
    stats[...] = jnp.where(lane == 0, highest, jnp.where(lane == 1, total, landed))


def finish(masked, received, queries, result, stats, logprob, attended, values, sems):
    lines = received[:, 8, :].astype(F32)
    take = lambda k: lines[:, 32 * k : 32 * (k + 1)]
    peak, total = take(0), take(1) + take(2) + take(3)
    highest = jnp.max(peak, axis=0, keepdims=True)
    total = jnp.sum(total * jnp.exp(peak - highest), axis=0, keepdims=True)
    normalizer = highest + jnp.log(total)
    row, lane = iota((32, 32), 0), iota((32, 32), 1)
    normalizer = jnp.sum(jnp.where(row == lane, normalizer, 0.0), axis=1, keepdims=True)
    copies = []
    for b in range(4):
        at = slice(BLK * b, BLK * (b + 1))
        section = masked[:, at].astype(F32)
        values[:, at] = jnp.where(section == -jnp.inf, 0.0, section - normalizer)
        piece = pl.ds(BLK * b, BLK)
        copies.append(
            pltpu.make_async_copy(values.at[:, piece], logprob.at[:, piece], sems.at[b])
        )
        copies[-1].start()
    row = iota((128, 1), 0)
    head, request = row // 32, row % 32
    query = jnp.concatenate([queries[:, HD * i : HD * (i + 1)] for i in range(4)], axis=0)
    table = received[...].reshape(256, HD)
    slot = (request // 2) * 16
    target = jnp.concatenate([slot, slot + 1, slot + (request % 2) * 4 + head], axis=0)
    picked = pick(target, table)
    own_key, own_value, cached = picked[0:128], picked[128:256], picked[256:384]
    own = jnp.sum(query.astype(F32) * own_key, axis=1, keepdims=True) * SCALE
    top, total, landed = stats[:, 0:1], stats[:, 1:2], stats[:, 2:3]
    highest = jnp.maximum(top, own)
    share, own_share = jnp.exp(top - highest), jnp.exp(own - highest)
    scale = 1.0 / (total * share + own_share)
    merged = (result[...] * share + own_value * own_share) * scale
    merged = jnp.where(landed > 0.5, merged, cached).astype(BF16)
    for i in range(4):
        attended[:, HD * i : HD * (i + 1)] = merged[32 * i : 32 * (i + 1)]
    for copy in copies:
        copy.wait()


def exchanged(slots, axis):
    return lax.all_to_all(slots, axis, 0, 0, tiled=True)


def per_device(
    hidden,
    w_kv,
    prompt_lengths,
    owner_step,
    cache,
    cache_len,
    queries,
    fresh,
    logits,
    states,
    masks,
):
    vmem = pl.BlockSpec(memory_space=pltpu.VMEM)
    hbm = pl.BlockSpec(memory_space=pl.ANY)
    sent = jax.ShapeDtypeStruct
    kept = pltpu.VMEM
    held = lambda *values: [
        pltpu.with_memory_space_constraint(value, pltpu.VMEM) for value in values
    ]
    tokens, wide = hidden.shape[0] // 4, hidden.shape[1]
    *shares, asked = pl.pallas_call(
        prepare,
        out_shape=[kept((tokens, wide), BF16)] * 4 + [kept((16, 16, HD), BF16)],
        in_specs=[hbm] * 3,
        out_specs=[vmem] * 5,
        scratch_shapes=[
            pltpu.VMEM(queries.shape, BF16),
            pltpu.VMEM(fresh.shape, BF16),
            pltpu.SemaphoreType.DMA((6,)),
        ],
        name="prepare",
    )(hidden, queries, fresh)
    for k in (1, 3, 2):
        shares[k] = lax.ppermute(shares[k], "x", [(0, k)])
    weight = pl.pallas_call(
        fetch,
        out_shape=kept(w_kv.shape, BF16),
        in_specs=[hbm],
        out_specs=vmem,
        scratch_shapes=[pltpu.SemaphoreType.DMA],
        name="fetch",
    )(w_kv)
    projected = pl.pallas_call(
        project,
        out_shape=sent((16, 80, HD), BF16),
        in_specs=[vmem] * 6,
        out_specs=hbm,
        scratch_shapes=[pltpu.VMEM((16, 80, HD), BF16), pltpu.SemaphoreType.DMA((4,))],
        name="project",
    )(*held(*shares, asked, weight))
    pieces = exchanged(projected, TP)
    masked, terms = pl.pallas_call(
        grammar,
        out_shape=[kept(logits.shape, BF16), kept((16, HD), BF16)],
        in_specs=[vmem] * 3,
        out_specs=[vmem] * 2,
        name="grammar",
    )(*held(logits, states.reshape(1, -1), masks))
    block = pl.pallas_call(
        reduce_blocks,
        out_shape=kept((tokens, HD), BF16),
        in_specs=[vmem],
        out_specs=vmem,
        name="reduce",
    )(*held(pieces))
    other = lax.ppermute(block, "zl", [(0, 1), (1, 0)])
    answers = pl.pallas_call(
        attend_cached,
        out_shape=sent((16, 16, HD), BF16),
        in_specs=[vmem] * 6,
        name="cached",
    )(*held(cache_len.reshape(1, 2), pieces, cache, terms, prompt_lengths, owner_step))
    answers = exchanged(answers, TP)
    both = jnp.concatenate([block, other], axis=0)
    around = lax.all_gather(both, "x")
    result, stats = pl.pallas_call(
        attend_prompts,
        out_shape=[kept((128, HD), F32), kept((128, HD), F32)],
        in_specs=[vmem] * 4,
        out_specs=[vmem] * 2,
        name="prompts",
    )(*held(around, queries, prompt_lengths, owner_step))
    logprob, attended = pl.pallas_call(
        finish,
        out_shape=[sent(logits.shape, F32), sent(queries.shape, BF16)],
        in_specs=[vmem] * 5,
        out_specs=[hbm, vmem],
        scratch_shapes=[pltpu.VMEM(logits.shape, F32), pltpu.SemaphoreType.DMA((4,))],
        name="finish",
    )(*held(masked, answers, queries, result, stats))
    return attended, logprob


def solution(mesh):
    groups, columns = mesh.shape["group"], mesh.shape["tp"]
    finer = Mesh(
        mesh.devices.reshape(4, groups // 4, columns // 2, 2), ("x", "c8", "zh", "zl")
    )
    group = ("x", "c8")
    in_specs = (
        P(group, TP),
        P(TP, None),
        P(),
        P(),
        P(group + TP, None, None),
        P(group + TP),
        P(group, TP),
        P(group, TP),
        P(group, TP),
        P(group),
        P(None, TP),
    )
    return jax.shard_map(
        per_device,
        mesh=finer,
        in_specs=in_specs,
        out_specs=(P(group, TP), P(group, TP)),
        check_vma=False,
    )
```

```python
import math

import jax
import jax.numpy as jnp
from jax import lax
from jax.experimental import pallas as pl
from jax.experimental.pallas import tpu as pltpu
from jax.sharding import Mesh, PartitionSpec as P

KVH = 8
HD = 128
STATES = 24
BITS = 30
LOWEST = -1e30
BLK = 1920
SCALE = 1.0 / math.sqrt(HD)
F32 = jnp.float32
BF16 = jnp.bfloat16
I32 = jnp.int32
TP = ("zh", "zl")


def iota(shape, dim):
    return lax.broadcasted_iota(I32, shape, dim)


def one_hot(target, width):
    rows = target.shape[0]
    return (iota((rows, width), 1) == target).astype(F32).astype(BF16)


def kernel(body, **options):
    limit = pltpu.CompilerParams(vmem_limit_bytes=16 << 20)
    return pl.pallas_call(body, compiler_params=limit, **options)


def pick(target, table):
    return jnp.dot(one_hot(target, table.shape[0]), table, preferred_element_type=F32)


def prompts_of(lengths, owners, source, turn):
    count = lengths.shape[1]
    here = iota(lengths.shape, 0) == source
    length = jnp.sum(jnp.where(here, lengths, 0).astype(F32), axis=0, keepdims=True)
    owner = jnp.sum(jnp.where(here, owners, 0).astype(F32), axis=0, keepdims=True)
    chosen = ((owner == turn.astype(F32)) & (turn >= 1)).astype(F32)
    row, lane = iota((count, count), 0), iota((count, count), 1)

    def before(values):
        column = jnp.sum(jnp.where(row == lane, values, 0.0), axis=1, keepdims=True)
        return jnp.sum(jnp.where(row < lane, column, 0.0), axis=0, keepdims=True)

    return chosen, before(chosen), before(length), length


def landing(slot, prompts):
    chosen, rank, start, length = prompts
    matched = jnp.where(rank == slot.astype(F32), chosen, 0.0)
    total = lambda values: jnp.sum(matched * values, axis=1, keepdims=True)
    return jnp.sum(matched, axis=1, keepdims=True), total(start), total(length)


def cut(hidden, own, first, second, third, sems):
    copies = [
        pltpu.make_async_copy(hidden.at[pl.ds(64 * k, 64)], out, sems.at[k])
        for k, out in enumerate((own, first, second, third))
    ]
    for copy in copies:
        copy.start()
    for copy in copies:
        copy.wait()


def pack(queries, fresh, out):
    table = jnp.concatenate(
        [queries[:, HD * i : HD * (i + 1)] for i in range(4)] + [fresh[...]], axis=0
    )
    row = iota((256, 1), 0)
    dest, k = row // 16, row % 16
    target = jnp.where(
        k < 8,
        (k % 4) * 32 + 2 * dest + k // 4,
        jnp.where(k < 10, 128 + 2 * dest + k - 8, 160),
    )
    out[...] = pick(target, table).astype(BF16).reshape(16, 16, HD)


def project(own, first, second, third, asked, weight, out, slots, sems):
    turn = lax.axis_index("x")
    tokens = jnp.where(turn == 0, own[...], first[...] + second[...] + third[...])
    slots[:, 64:80] = asked[...]
    copies = []
    for h in range(4):
        for part in range(2):
            at = HD * (KVH * part + 2 * h)
            full = jnp.dot(
                tokens, weight[:, at : at + 2 * HD], preferred_element_type=F32
            ).astype(BF16)
            slots[4 * h + part, 0:64] = full[:, :HD]
            slots[4 * h + 2 + part, 0:64] = full[:, HD:]
        four = pl.ds(4 * h, 4)
        copies.append(pltpu.make_async_copy(slots.at[four], out.at[four], sems.at[h]))
        copies[-1].start()
    for copy in copies:
        copy.wait()


def reduce_blocks(pieces, out):
    total = pieces[0, 0:64].astype(F32)
    for c in range(1, 16):
        total = total + pieces[c, 0:64].astype(F32)
    out[...] = total.astype(BF16)


def grammar(logits, states, masks, masked, terms):
    lane = iota((STATES, HD), 1)
    blocks = []
    for half in range(2):
        words = masks[:, HD * half : HD * (half + 1)]
        turned = pltpu.roll(words, 64, 1)
        for x, y in ((words, turned), (turned, words)):
            byte = lambda v, j: jnp.bitwise_and(jnp.right_shift(v, 8 * j), 255)
            blocks.append(
                jnp.concatenate(
                    [
                        jnp.where(lane < 64, byte(x, 0), byte(y, 1)),
                        jnp.where(lane < 64, byte(x, 2), byte(y, 3)),
                    ],
                    axis=1,
                )
            )
    table = jnp.concatenate(blocks, axis=0).astype(F32).astype(BF16)
    row, lane = iota((32, 32), 0), iota((32, 32), 1)
    state = jnp.where(row == lane, states[...], 0).astype(F32)
    state = jnp.sum(state, axis=1, keepdims=True).astype(I32)
    key = jnp.concatenate([state + STATES * b for b in range(4)], axis=0)
    chosen = pick(key, table).astype(BF16)
    column = iota((1, BLK), 1)
    word = jnp.right_shift(column * 34953, 20)
    bit = column - word * BITS
    wanted = jnp.right_shift(bit, 3) * 64 + word
    flag = jnp.left_shift(jnp.ones_like(bit), jnp.bitwise_and(bit, 7))
    spread = (iota((256, BLK), 0) == wanted).astype(F32).astype(BF16)
    peak = None
    kept = []
    for b in range(4):
        value = jnp.dot(
            chosen[32 * b : 32 * (b + 1)], spread, preferred_element_type=F32
        ).astype(I32)
        section = logits[:, BLK * b : BLK * (b + 1)].astype(F32)
        section = jnp.where(jnp.bitwise_and(value, flag) != 0, section, -jnp.inf)
        kept.append(section)
        masked[:, BLK * b : BLK * (b + 1)] = section.astype(BF16)
        top = jnp.max(section, axis=1, keepdims=True)
        peak = top if peak is None else jnp.maximum(peak, top)
    total = sum(jnp.sum(jnp.exp(section - peak), axis=1, keepdims=True) for section in kept)
    high = total.astype(BF16).astype(F32)
    middle = (total - high).astype(BF16).astype(F32)
    low = total - high - middle
    row, lane = iota((32, HD), 0), iota((32, HD), 1)
    spot = lane - row
    line = jnp.where(
        spot == 0, peak, jnp.where(spot == 32, high, jnp.where(spot == 64, middle, low))
    )
    line = jnp.where(jnp.bitwise_and(spot, 31) == 0, line, 0.0)
    terms[...] = jnp.broadcast_to(jnp.sum(line, axis=0, keepdims=True), (16, HD)).astype(BF16)


def softmax(score, own, alive):
    highest = jnp.maximum(
        jnp.max(jnp.where(alive, score, -jnp.inf), axis=1, keepdims=True), own
    )
    exponent = jnp.where(alive, jnp.exp(score - highest), 0.0)
    own_exponent = jnp.exp(own - highest)
    total = jnp.sum(exponent, axis=1, keepdims=True) + own_exponent
    own_weight = (own_exponent / total).astype(BF16).astype(F32)
    return (exponent / total).astype(BF16), own_weight


def transposed(a, b):
    return lax.dot_general(a, b, (((1,), (1,)), ((), ())), preferred_element_type=F32)


def attend_cached(cache_len, received, cache, terms, lengths, owners, out):
    column = lax.axis_index("zh") * 2 + lax.axis_index("zl")
    prompts = prompts_of(
        lengths[...], owners[...], lax.axis_index("c8"), lax.axis_index("x")
    )
    landed = landing(jnp.full((1, 1), column, I32), prompts)[0]
    table = received[:, 64:80, :].reshape(256, HD)
    row = iota((256, 1), 0)
    device, k = row // 16, row % 16
    second = (k >= 4) & (k < 8)
    fresh_row = (device // 2) * 16 + jnp.where(second, 9, 8)
    own_key = pick(fresh_row, table)
    own_value = pick(fresh_row + KVH * 16, table)
    own = jnp.sum(table.astype(F32) * own_key, axis=1, keepdims=True) * SCALE
    second32 = second[0:32]
    scores = []
    for h in range(KVH):
        rows = table[32 * h : 32 * (h + 1)]
        both = [transposed(rows, cache[r, :, HD * h : HD * (h + 1)]) for r in range(2)]
        scores.append(jnp.where(second32, both[1], both[0]))
    score = jnp.concatenate(scores, axis=0) * SCALE
    alive = iota((256, HD), 1) < jnp.where(second, cache_len[0:1, 1:2], cache_len[0:1, 0:1])
    weight, own_weight = softmax(score, own, alive)
    values = []
    for h in range(KVH):
        rows = weight[32 * h : 32 * (h + 1)]
        at = HD * (KVH + h)
        both = [
            jnp.dot(rows, cache[r, :, at : at + HD], preferred_element_type=F32)
            for r in range(2)
        ]
        values.append(jnp.where(second32, both[1], both[0]))
    result = jnp.concatenate(values, axis=0) + own_weight * own_value
    arrived = jnp.broadcast_to(landed > 0.5, (256, 1))
    result = jnp.where(arrived & (k == 0), own_key, result)
    result = jnp.where(arrived & (k == 1), own_value, result)
    result = jnp.where(k == 8, terms[0:1, :].astype(F32), result)
    out[...] = result.astype(BF16).reshape(16, 16, HD)


def attend_prompts(parts, queries, lengths, owners, result, stats):
    prompts = prompts_of(
        lengths[...], owners[...], lax.axis_index("c8"), lax.axis_index("x")
    )
    request = iota((128, 1), 0) % 32
    landed, start, length = landing((request % 2) * 16 + request // 2, prompts)
    even = lax.axis_index("zl") == 0
    mine = jnp.concatenate([parts[x, 0:64] for x in range(4)], axis=0)
    other = jnp.concatenate([parts[x, 64:128] for x in range(4)], axis=0)
    keys = jnp.where(even, mine, other)
    values = jnp.where(even, other, mine)
    query = jnp.concatenate([queries[:, HD * i : HD * (i + 1)] for i in range(4)], axis=0)
    score = transposed(query, keys) * SCALE
    position = iota((128, 256), 1).astype(F32)
    alive = (position >= start) & (position < start + length)
    highest = jnp.max(jnp.where(alive, score, LOWEST), axis=1, keepdims=True)
    exponent = jnp.where(alive, jnp.exp(score - highest), 0.0)
    result[...] = jnp.dot(exponent.astype(BF16), values, preferred_element_type=F32)
    total = jnp.sum(exponent, axis=1, keepdims=True)
    lane = iota((128, HD), 1)
    stats[...] = jnp.where(lane == 0, highest, jnp.where(lane == 1, total, landed))


def finish(masked, received, queries, result, stats, logprob, attended, values, sems):
    lines = received[:, 8, :].astype(F32)
    take = lambda k: lines[:, 32 * k : 32 * (k + 1)]
    peak, total = take(0), take(1) + take(2) + take(3)
    highest = jnp.max(peak, axis=0, keepdims=True)
    total = jnp.sum(total * jnp.exp(peak - highest), axis=0, keepdims=True)
    normalizer = highest + jnp.log(total)
    row, lane = iota((32, 32), 0), iota((32, 32), 1)
    normalizer = jnp.sum(jnp.where(row == lane, normalizer, 0.0), axis=1, keepdims=True)
    row = iota((128, 1), 0)
    head, request = row // 32, row % 32
    query = jnp.concatenate([queries[:, HD * i : HD * (i + 1)] for i in range(4)], axis=0)
    table = received[...].reshape(256, HD)
    slot = (request // 2) * 16
    target = jnp.concatenate([slot, slot + 1, slot + (request % 2) * 4 + head], axis=0)
    picked = pick(target, table)
    own_key, own_value, cached = picked[0:128], picked[128:256], picked[256:384]
    own = jnp.sum(query.astype(F32) * own_key, axis=1, keepdims=True) * SCALE
    top, total, landed = stats[:, 0:1], stats[:, 1:2], stats[:, 2:3]
    highest = jnp.maximum(top, own)
    share, own_share = jnp.exp(top - highest), jnp.exp(own - highest)
    scale = 1.0 / (total * share + own_share)
    merged = (result[...] * share + own_value * own_share) * scale
    merged = jnp.where(landed > 0.5, merged, cached).astype(BF16)
    copies = []
    for b in range(4):
        at = slice(BLK * b, BLK * (b + 1))
        section = masked[:, at].astype(F32)
        values[:, at] = jnp.where(section == -jnp.inf, 0.0, section - normalizer)
        piece = pl.ds(BLK * b, BLK)
        copies.append(
            pltpu.make_async_copy(values.at[:, piece], logprob.at[:, piece], sems.at[b])
        )
        copies[-1].start()
    for i in range(4):
        attended[:, HD * i : HD * (i + 1)] = merged[32 * i : 32 * (i + 1)]
    for copy in copies:
        copy.wait()


def exchanged(slots, axis):
    return lax.all_to_all(slots, axis, 0, 0, tiled=True)


def per_device(
    hidden,
    w_kv,
    prompt_lengths,
    owner_step,
    cache,
    cache_len,
    queries,
    fresh,
    logits,
    states,
    masks,
):
    vmem = pl.BlockSpec(memory_space=pltpu.VMEM)
    hbm = pl.BlockSpec(memory_space=pltpu.HBM)
    sent = jax.ShapeDtypeStruct
    kept = pltpu.VMEM
    held = lambda *values: [
        pltpu.with_memory_space_constraint(value, pltpu.VMEM) for value in values
    ]
    tokens, wide = hidden.shape[0] // 4, hidden.shape[1]
    shares = list(kernel(
        cut,
        out_shape=[kept((tokens, wide), BF16)] * 4,
        in_specs=[hbm],
        out_specs=[vmem] * 4,
        scratch_shapes=[pltpu.SemaphoreType.DMA((4,))],
        name="cut",
        cost_estimate=pl.CostEstimate(flops=2000000000, bytes_accessed=1000, transcendentals=0),
    )(pltpu.with_memory_space_constraint(hidden, pltpu.HBM)))
    for k in (1, 3, 2):
        shares[k] = lax.ppermute(shares[k], "x", [(0, k)])
    asked = kernel(
        pack,
        out_shape=kept((16, 16, HD), BF16),
        in_specs=[vmem] * 2,
        out_specs=vmem,
        name="pack",
    )(*held(queries, fresh))
    projected = kernel(
        project,
        out_shape=pltpu.HBM((16, 80, HD), BF16),
        in_specs=[vmem] * 6,
        out_specs=hbm,
        scratch_shapes=[pltpu.VMEM((16, 80, HD), BF16), pltpu.SemaphoreType.DMA((4,))],
        name="project",
    )(*held(*shares, asked, w_kv))
    pieces = exchanged(projected, TP)
    masked, terms = kernel(
        grammar,
        out_shape=[kept(logits.shape, BF16), kept((16, HD), BF16)],
        in_specs=[vmem] * 3,
        out_specs=[vmem] * 2,
        name="grammar",
    )(*held(logits, states.reshape(1, -1), masks))
    block = kernel(
        reduce_blocks,
        out_shape=kept((tokens, HD), BF16),
        in_specs=[vmem],
        out_specs=vmem,
        name="reduce",
    )(*held(pieces))
    other = lax.ppermute(block, "zl", [(0, 1), (1, 0)])
    answers = kernel(
        attend_cached,
        out_shape=sent((16, 16, HD), BF16),
        in_specs=[vmem] * 6,
        name="cached",
    )(*held(cache_len.reshape(1, 2), pieces, cache, terms, prompt_lengths, owner_step))
    answers = exchanged(answers, TP)
    both = jnp.concatenate([block, other], axis=0)
    around = lax.all_gather(both, "x")
    result, stats = kernel(
        attend_prompts,
        out_shape=[kept((128, HD), F32), kept((128, HD), F32)],
        in_specs=[vmem] * 4,
        out_specs=[vmem] * 2,
        name="prompts",
    )(*held(around, queries, prompt_lengths, owner_step))
    logprob, attended = kernel(
        finish,
        out_shape=[pltpu.HBM(logits.shape, F32), sent(queries.shape, BF16)],
        in_specs=[vmem] * 5,
        out_specs=[hbm, vmem],
        scratch_shapes=[pltpu.VMEM(logits.shape, F32), pltpu.SemaphoreType.DMA((4,))],
        name="finish",
    )(*held(masked, answers, queries, result, stats))
    return attended, logprob


def solution(mesh):
    groups, columns = mesh.shape["group"], mesh.shape["tp"]
    finer = Mesh(
        mesh.devices.reshape(4, groups // 4, columns // 2, 2), ("x", "c8", "zh", "zl")
    )
    group = ("x", "c8")
    in_specs = (
        P(group, TP),
        P(TP, None),
        P(),
        P(),
        P(group + TP, None, None),
        P(group + TP),
        P(group, TP),
        P(group, TP),
        P(group, TP),
        P(group),
        P(None, TP),
    )
    return jax.shard_map(
        per_device,
        mesh=finer,
        in_specs=in_specs,
        out_specs=(P(group, TP), P(group, TP)),
        check_vma=False,
    )
```

```python
import math

import jax
import jax.numpy as jnp
from jax import lax
from jax.experimental import pallas as pl
from jax.experimental.pallas import tpu as pltpu
from jax.sharding import Mesh, PartitionSpec as P

KVH = 8
HD = 128
STATES = 24
BITS = 30
LOWEST = -1e30
BLK = 1920
SCALE = 1.0 / math.sqrt(HD)
F32 = jnp.float32
BF16 = jnp.bfloat16
I32 = jnp.int32
TP = ("zh", "zl")


def iota(shape, dim):
    return lax.broadcasted_iota(I32, shape, dim)


def one_hot(target, width):
    rows = target.shape[0]
    return (iota((rows, width), 1) == target).astype(F32).astype(BF16)


def kernel(body, **options):
    limit = pltpu.CompilerParams(vmem_limit_bytes=16 << 20)
    return pl.pallas_call(body, compiler_params=limit, **options)


def pick(target, table):
    return jnp.dot(one_hot(target, table.shape[0]), table, preferred_element_type=F32)


def prompts_of(lengths, owners, source, turn):
    count = lengths.shape[1]
    here = iota(lengths.shape, 0) == source
    length = jnp.sum(jnp.where(here, lengths, 0).astype(F32), axis=0, keepdims=True)
    owner = jnp.sum(jnp.where(here, owners, 0).astype(F32), axis=0, keepdims=True)
    chosen = ((owner == turn.astype(F32)) & (turn >= 1)).astype(F32)
    row, lane = iota((count, count), 0), iota((count, count), 1)

    def before(values):
        column = jnp.sum(jnp.where(row == lane, values, 0.0), axis=1, keepdims=True)
        return jnp.sum(jnp.where(row < lane, column, 0.0), axis=0, keepdims=True)

    return chosen, before(chosen), before(length), length


def landing(slot, prompts):
    chosen, rank, start, length = prompts
    matched = jnp.where(rank == slot.astype(F32), chosen, 0.0)
    total = lambda values: jnp.sum(matched * values, axis=1, keepdims=True)
    return jnp.sum(matched, axis=1, keepdims=True), total(start), total(length)


def cut(hidden, own, first, second, third, sems):
    copies = [
        pltpu.make_async_copy(hidden.at[pl.ds(64 * k, 64)], out, sems.at[k])
        for k, out in enumerate((own, first, second, third))
    ]
    for copy in copies:
        copy.start()
    for copy in copies:
        copy.wait()


def pack(queries, out):
    table = jnp.concatenate([queries[:, HD * i : HD * (i + 1)] for i in range(4)], axis=0)
    row = iota((128, 1), 0)
    dest, k = row // 8, row % 8
    out[...] = pick((k % 4) * 32 + 2 * dest + k // 4, table).astype(BF16).reshape(16, 8, HD)


def project(own, first, second, third, asked, weight, out, slots, sems):
    turn = lax.axis_index("x")
    tokens = jnp.where(turn == 0, own[...], first[...] + second[...] + third[...])
    slots[:, 64:72] = asked[...]
    copies = []
    for h in range(4):
        for part in range(2):
            at = HD * (KVH * part + 2 * h)
            full = jnp.dot(
                tokens, weight[:, at : at + 2 * HD], preferred_element_type=F32
            ).astype(BF16)
            slots[4 * h + part, 0:64] = full[:, :HD]
            slots[4 * h + 2 + part, 0:64] = full[:, HD:]
        four = pl.ds(4 * h, 4)
        copies.append(pltpu.make_async_copy(slots.at[four], out.at[four], sems.at[h]))
        copies[-1].start()
    for copy in copies:
        copy.wait()


def reduce_blocks(pieces, out):
    total = pieces[0, 0:64].astype(F32)
    for c in range(1, 16):
        total = total + pieces[c, 0:64].astype(F32)
    out[...] = total.astype(BF16)


def grammar(logits, states, masks, masked, terms):
    lane = iota((STATES, HD), 1)
    blocks = []
    for half in range(2):
        words = masks[:, HD * half : HD * (half + 1)]
        turned = pltpu.roll(words, 64, 1)
        for x, y in ((words, turned), (turned, words)):
            byte = lambda v, j: jnp.bitwise_and(jnp.right_shift(v, 8 * j), 255)
            blocks.append(
                jnp.concatenate(
                    [
                        jnp.where(lane < 64, byte(x, 0), byte(y, 1)),
                        jnp.where(lane < 64, byte(x, 2), byte(y, 3)),
                    ],
                    axis=1,
                )
            )
    table = jnp.concatenate(blocks, axis=0).astype(F32).astype(BF16)
    row, lane = iota((32, 32), 0), iota((32, 32), 1)
    state = jnp.where(row == lane, states[...], 0).astype(F32)
    state = jnp.sum(state, axis=1, keepdims=True).astype(I32)
    key = jnp.concatenate([state + STATES * b for b in range(4)], axis=0)
    chosen = pick(key, table).astype(BF16)
    column = iota((1, BLK), 1)
    word = jnp.right_shift(column * 34953, 20)
    bit = column - word * BITS
    wanted = jnp.right_shift(bit, 3) * 64 + word
    flag = jnp.left_shift(jnp.ones_like(bit), jnp.bitwise_and(bit, 7))
    spread = (iota((256, BLK), 0) == wanted).astype(F32).astype(BF16)
    peak = None
    kept = []
    for b in range(4):
        value = jnp.dot(
            chosen[32 * b : 32 * (b + 1)], spread, preferred_element_type=F32
        ).astype(I32)
        section = logits[:, BLK * b : BLK * (b + 1)].astype(F32)
        section = jnp.where(jnp.bitwise_and(value, flag) != 0, section, -jnp.inf)
        kept.append(section)
        masked[:, BLK * b : BLK * (b + 1)] = section.astype(BF16)
        top = jnp.max(section, axis=1, keepdims=True)
        peak = top if peak is None else jnp.maximum(peak, top)
    total = sum(jnp.sum(jnp.exp(section - peak), axis=1, keepdims=True) for section in kept)
    high, middle, low = thirds(total)
    row, lane = iota((32, HD), 0), iota((32, HD), 1)
    spot = lane - row
    line = jnp.where(
        spot == 0, peak, jnp.where(spot == 32, high, jnp.where(spot == 64, middle, low))
    )
    line = jnp.where(jnp.bitwise_and(spot, 31) == 0, line, 0.0)
    terms[...] = jnp.broadcast_to(jnp.sum(line, axis=0, keepdims=True), (16, HD)).astype(BF16)


def transposed(a, b):
    return lax.dot_general(a, b, (((1,), (1,)), ((), ())), preferred_element_type=F32)


def thirds(value):
    high = value.astype(BF16).astype(F32)
    middle = (value - high).astype(BF16).astype(F32)
    return high, middle, value - high - middle


def attend_cached(cache_len, received, cache, terms, out):
    table = received[:, 64:72, :].reshape(128, HD)
    k = iota((128, 1), 0) % 8
    second = k >= 4
    second16 = second[0:16]
    scores = []
    for h in range(KVH):
        rows = table[16 * h : 16 * (h + 1)]
        both = [transposed(rows, cache[r, :, HD * h : HD * (h + 1)]) for r in range(2)]
        scores.append(jnp.where(second16, both[1], both[0]))
    score = jnp.concatenate(scores, axis=0) * SCALE
    count = jnp.where(second, cache_len[0:1, 1:2], cache_len[0:1, 0:1])
    alive = iota((128, HD), 1) < count
    highest = jnp.max(jnp.where(alive, score, LOWEST), axis=1, keepdims=True)
    exponent = jnp.where(alive, jnp.exp(score - highest), 0.0)
    total = jnp.sum(exponent, axis=1, keepdims=True)
    weight = (exponent / total).astype(BF16)
    values = []
    for h in range(KVH):
        rows = weight[16 * h : 16 * (h + 1)]
        at = HD * (KVH + h)
        both = [
            jnp.dot(rows, cache[r, :, at : at + HD], preferred_element_type=F32)
            for r in range(2)
        ]
        values.append(jnp.where(second16, both[1], both[0]))
    high, middle, low = thirds(highest + jnp.log(total))
    spot = iota((128, HD), 1) - k
    line = jnp.where(
        spot == 0, high, jnp.where(spot == 8, middle, jnp.where(spot == 16, low, 0.0))
    )
    line = jnp.sum(line.reshape(16, 8, HD), axis=1, keepdims=True)
    slot = iota((16, 8, HD), 1)
    rest = jnp.where(slot == 0, terms[0:1, :].astype(F32).reshape(1, 1, HD), line)
    result = jnp.concatenate(values, axis=0).reshape(16, 8, HD)
    out[...] = jnp.concatenate([result, rest], axis=1).astype(BF16)


def attend_prompts(parts, queries, lengths, owners, result, stats):
    prompts = prompts_of(
        lengths[...], owners[...], lax.axis_index("c8"), lax.axis_index("x")
    )
    request = iota((128, 1), 0) % 32
    landed, start, length = landing((request % 2) * 16 + request // 2, prompts)
    even = lax.axis_index("zl") == 0
    mine = jnp.concatenate([parts[x, 0:64] for x in range(4)], axis=0)
    other = jnp.concatenate([parts[x, 64:128] for x in range(4)], axis=0)
    keys = jnp.where(even, mine, other)
    values = jnp.where(even, other, mine)
    query = jnp.concatenate([queries[:, HD * i : HD * (i + 1)] for i in range(4)], axis=0)
    score = transposed(query, keys) * SCALE
    position = iota((128, 256), 1).astype(F32)
    alive = (position >= start) & (position < start + length)
    highest = jnp.max(jnp.where(alive, score, LOWEST), axis=1, keepdims=True)
    exponent = jnp.where(alive, jnp.exp(score - highest), 0.0)
    result[...] = jnp.dot(exponent.astype(BF16), values, preferred_element_type=F32)
    total = jnp.sum(exponent, axis=1, keepdims=True)
    lane = iota((128, HD), 1)
    stats[...] = jnp.where(lane == 0, highest, jnp.where(lane == 1, total, landed))


def finish(masked, received, queries, first, second, result, stats, logprob, attended, values, sems):
    lines = received[:, 8, :].astype(F32)
    take = lambda k: lines[:, 32 * k : 32 * (k + 1)]
    peak, total = take(0), take(1) + take(2) + take(3)
    highest = jnp.max(peak, axis=0, keepdims=True)
    total = jnp.sum(total * jnp.exp(peak - highest), axis=0, keepdims=True)
    normalizer = highest + jnp.log(total)
    row, lane = iota((32, 32), 0), iota((32, 32), 1)
    normalizer = jnp.sum(jnp.where(row == lane, normalizer, 0.0), axis=1, keepdims=True)
    row = iota((128, 1), 0)
    head, request = row // 32, row % 32
    query = jnp.concatenate([queries[:, HD * i : HD * (i + 1)] for i in range(4)], axis=0)
    table = received[...].reshape(256, HD)
    place = (request % 2) * 4 + head
    slot = (request // 2) * 16
    picked = pick(jnp.concatenate([slot + place, slot + 9], axis=0), table)
    spot = iota((128, HD), 1) - place
    cached_top = jnp.where((spot == 0) | (spot == 8) | (spot == 16), picked[128:256], 0.0)
    cached_top = jnp.sum(cached_top, axis=1, keepdims=True)
    even = lax.axis_index("zl") == 0
    own_key = jnp.where(even, first[...], second[...]).astype(F32)
    own_value = jnp.where(even, second[...], first[...]).astype(F32)
    own_key = jnp.concatenate([own_key] * 4, axis=0)
    own_value = jnp.concatenate([own_value] * 4, axis=0)
    own = jnp.sum(query.astype(F32) * own_key, axis=1, keepdims=True) * SCALE
    landed = stats[:, 2:3] > 0.5
    top = jnp.where(landed, stats[:, 0:1], cached_top)
    total = jnp.where(landed, stats[:, 1:2], 1.0)
    live = jnp.where(landed, result[...], picked[0:128])
    highest = jnp.maximum(top, own)
    share, own_share = jnp.exp(top - highest), jnp.exp(own - highest)
    scale = 1.0 / (total * share + own_share)
    merged = ((live * share + own_value * own_share) * scale).astype(BF16)
    copies = []
    for b in range(4):
        at = slice(BLK * b, BLK * (b + 1))
        section = masked[:, at].astype(F32)
        values[:, at] = jnp.where(section == -jnp.inf, 0.0, section - normalizer)
        piece = pl.ds(BLK * b, BLK)
        copies.append(
            pltpu.make_async_copy(values.at[:, piece], logprob.at[:, piece], sems.at[b])
        )
        copies[-1].start()
    for i in range(4):
        attended[:, HD * i : HD * (i + 1)] = merged[32 * i : 32 * (i + 1)]
    for copy in copies:
        copy.wait()


def exchanged(slots, axis):
    return lax.all_to_all(slots, axis, 0, 0, tiled=True)


def per_device(
    hidden,
    w_kv,
    prompt_lengths,
    owner_step,
    cache,
    cache_len,
    queries,
    fresh,
    logits,
    states,
    masks,
):
    vmem = pl.BlockSpec(memory_space=pltpu.VMEM)
    hbm = pl.BlockSpec(memory_space=pltpu.HBM)
    sent = jax.ShapeDtypeStruct
    kept = pltpu.VMEM
    held = lambda *values: [
        pltpu.with_memory_space_constraint(value, pltpu.VMEM) for value in values
    ]
    tokens, wide = hidden.shape[0] // 4, hidden.shape[1]
    shares = list(kernel(
        cut,
        out_shape=[kept((tokens, wide), BF16)] * 4,
        in_specs=[hbm],
        out_specs=[vmem] * 4,
        scratch_shapes=[pltpu.SemaphoreType.DMA((4,))],
        name="cut",
        cost_estimate=pl.CostEstimate(flops=2000000000, bytes_accessed=1000, transcendentals=0),
    )(pltpu.with_memory_space_constraint(hidden, pltpu.HBM)))
    for k in (1, 3, 2):
        shares[k] = lax.ppermute(shares[k], "x", [(0, k)])
    asked = kernel(
        pack,
        out_shape=kept((16, 8, HD), BF16),
        in_specs=[vmem],
        out_specs=vmem,
        name="pack",
    )(*held(queries))
    projected = kernel(
        project,
        out_shape=pltpu.HBM((16, 72, HD), BF16),
        in_specs=[vmem] * 6,
        out_specs=hbm,
        scratch_shapes=[pltpu.VMEM((16, 72, HD), BF16), pltpu.SemaphoreType.DMA((4,))],
        name="project",
    )(*held(*shares, asked, w_kv))
    pieces = exchanged(projected, TP)
    keys_first = [(b, 2 * b) if b < KVH else (b, 2 * (b - KVH) + 1) for b in range(16)]
    values_first = [(b, d + 1 - 2 * (d % 2)) for b, d in keys_first]
    renewed = [lax.ppermute(fresh, TP, route) for route in (keys_first, values_first)]
    masked, terms = kernel(
        grammar,
        out_shape=[kept(logits.shape, BF16), kept((16, HD), BF16)],
        in_specs=[vmem] * 3,
        out_specs=[vmem] * 2,
        name="grammar",
    )(*held(logits, states.reshape(1, -1), masks))
    block = kernel(
        reduce_blocks,
        out_shape=kept((tokens, HD), BF16),
        in_specs=[vmem],
        out_specs=vmem,
        name="reduce",
    )(*held(pieces))
    other = lax.ppermute(block, "zl", [(0, 1), (1, 0)])
    answers = kernel(
        attend_cached,
        out_shape=sent((16, 16, HD), BF16),
        in_specs=[vmem] * 4,
        name="cached",
    )(*held(cache_len.reshape(1, 2), pieces, cache, terms))
    answers = exchanged(answers, TP)
    both = jnp.concatenate([block, other], axis=0)
    around = lax.all_gather(both, "x")
    result, stats = kernel(
        attend_prompts,
        out_shape=[kept((128, HD), F32), kept((128, HD), F32)],
        in_specs=[vmem] * 4,
        out_specs=[vmem] * 2,
        name="prompts",
    )(*held(around, queries, prompt_lengths, owner_step))
    logprob, attended = kernel(
        finish,
        out_shape=[pltpu.HBM(logits.shape, F32), sent(queries.shape, BF16)],
        in_specs=[vmem] * 7,
        out_specs=[hbm, vmem],
        scratch_shapes=[pltpu.VMEM(logits.shape, F32), pltpu.SemaphoreType.DMA((4,))],
        name="finish",
    )(*held(masked, answers, queries, *renewed, result, stats))
    return attended, logprob


def solution(mesh):
    groups, columns = mesh.shape["group"], mesh.shape["tp"]
    finer = Mesh(
        mesh.devices.reshape(4, groups // 4, columns // 2, 2), ("x", "c8", "zh", "zl")
    )
    group = ("x", "c8")
    in_specs = (
        P(group, TP),
        P(TP, None),
        P(),
        P(),
        P(group + TP, None, None),
        P(group + TP),
        P(group, TP),
        P(group, TP),
        P(group, TP),
        P(group),
        P(None, TP),
    )
    return jax.shard_map(
        per_device,
        mesh=finer,
        in_specs=in_specs,
        out_specs=(P(group, TP), P(group, TP)),
        check_vma=False,
    )
```

```python
import math

import jax
import jax.numpy as jnp
from jax import lax
from jax.experimental import pallas as pl
from jax.experimental.pallas import tpu as pltpu
from jax.sharding import Mesh, PartitionSpec as P

KVH = 8
HD = 128
STATES = 24
BITS = 30
LOWEST = -1e30
BLK = 1920
SCALE = 1.0 / math.sqrt(HD)
F32 = jnp.float32
BF16 = jnp.bfloat16
I32 = jnp.int32
TP = ("zh", "zl")


def iota(shape, dim):
    return lax.broadcasted_iota(I32, shape, dim)


def one_hot(target, width):
    rows = target.shape[0]
    return (iota((rows, width), 1) == target).astype(F32).astype(BF16)


def kernel(body, **options):
    limit = pltpu.CompilerParams(vmem_limit_bytes=16 << 20)
    return pl.pallas_call(body, compiler_params=limit, **options)


def pick(target, table):
    return jnp.dot(one_hot(target, table.shape[0]), table, preferred_element_type=F32)


def prompts_of(lengths, owners, source, turn):
    count = lengths.shape[1]
    here = iota(lengths.shape, 0) == source
    length = jnp.sum(jnp.where(here, lengths, 0).astype(F32), axis=0, keepdims=True)
    owner = jnp.sum(jnp.where(here, owners, 0).astype(F32), axis=0, keepdims=True)
    chosen = ((owner == turn.astype(F32)) & (turn >= 1)).astype(F32)
    row, lane = iota((count, count), 0), iota((count, count), 1)

    def before(values):
        column = jnp.sum(jnp.where(row == lane, values, 0.0), axis=1, keepdims=True)
        return jnp.sum(jnp.where(row < lane, column, 0.0), axis=0, keepdims=True)

    return chosen, before(chosen), before(length), length


def landing(slot, prompts):
    chosen, rank, start, length = prompts
    matched = jnp.where(rank == slot.astype(F32), chosen, 0.0)
    total = lambda values: jnp.sum(matched * values, axis=1, keepdims=True)
    return jnp.sum(matched, axis=1, keepdims=True), total(start), total(length)


def cut(hidden, own, first, second, third, sems):
    copies = [
        pltpu.make_async_copy(hidden.at[pl.ds(64 * k, 64)], out, sems.at[k])
        for k, out in enumerate((own, first, second, third))
    ]
    for copy in copies:
        copy.start()
    for copy in copies:
        copy.wait()


def pack(queries, out):
    table = jnp.concatenate([queries[:, HD * i : HD * (i + 1)] for i in range(4)], axis=0)
    row = iota((128, 1), 0)
    dest, k = row // 8, row % 8
    out[...] = pick((k % 4) * 32 + 2 * dest + k // 4, table).astype(BF16).reshape(16, 8, HD)


def project(own, first, second, third, asked, weight, out, slots, sems):
    turn = lax.axis_index("x")
    tokens = jnp.where(turn == 0, own[...], first[...] + second[...] + third[...])
    slots[:, 64:72] = asked[...]
    copies = []
    for h in range(4):
        for part in range(2):
            at = HD * (KVH * part + 2 * h)
            full = jnp.dot(
                tokens, weight[:, at : at + 2 * HD], preferred_element_type=F32
            ).astype(BF16)
            slots[4 * h + part, 0:64] = full[:, :HD]
            slots[4 * h + 2 + part, 0:64] = full[:, HD:]
        four = pl.ds(4 * h, 4)
        copies.append(pltpu.make_async_copy(slots.at[four], out.at[four], sems.at[h]))
        copies[-1].start()
    for copy in copies:
        copy.wait()


def reduce_blocks(pieces, out):
    total = pieces[0, 0:64].astype(F32)
    for c in range(1, 16):
        total = total + pieces[c, 0:64].astype(F32)
    out[...] = total.astype(BF16)


def grammar(logits, states, masks, masked, terms):
    lane = iota((STATES, HD), 1)
    blocks = []
    for half in range(2):
        words = masks[:, HD * half : HD * (half + 1)]
        turned = pltpu.roll(words, 64, 1)
        for x, y in ((words, turned), (turned, words)):
            byte = lambda v, j: jnp.bitwise_and(jnp.right_shift(v, 8 * j), 255)
            blocks.append(
                jnp.concatenate(
                    [
                        jnp.where(lane < 64, byte(x, 0), byte(y, 1)),
                        jnp.where(lane < 64, byte(x, 2), byte(y, 3)),
                    ],
                    axis=1,
                )
            )
    table = jnp.concatenate(blocks, axis=0).astype(F32).astype(BF16)
    row, lane = iota((32, 32), 0), iota((32, 32), 1)
    state = jnp.where(row == lane, states[...], 0).astype(F32)
    state = jnp.sum(state, axis=1, keepdims=True).astype(I32)
    key = jnp.concatenate([state + STATES * b for b in range(4)], axis=0)
    chosen = pick(key, table).astype(BF16)
    column = iota((1, BLK), 1)
    word = jnp.right_shift(column * 34953, 20)
    bit = column - word * BITS
    wanted = jnp.right_shift(bit, 3) * 64 + word
    flag = jnp.left_shift(jnp.ones_like(bit), jnp.bitwise_and(bit, 7))
    spread = (iota((256, BLK), 0) == wanted).astype(F32).astype(BF16)
    peak = None
    kept = []
    for b in range(4):
        value = jnp.dot(
            chosen[32 * b : 32 * (b + 1)], spread, preferred_element_type=F32
        ).astype(I32)
        section = logits[:, BLK * b : BLK * (b + 1)].astype(F32)
        section = jnp.where(jnp.bitwise_and(value, flag) != 0, section, -jnp.inf)
        kept.append(section)
        masked[:, BLK * b : BLK * (b + 1)] = section.astype(BF16)
        top = jnp.max(section, axis=1, keepdims=True)
        peak = top if peak is None else jnp.maximum(peak, top)
    total = sum(jnp.sum(jnp.exp(section - peak), axis=1, keepdims=True) for section in kept)
    high, middle, low = thirds(total)
    row, lane = iota((32, HD), 0), iota((32, HD), 1)
    spot = lane - row
    line = jnp.where(
        spot == 0, peak, jnp.where(spot == 32, high, jnp.where(spot == 64, middle, low))
    )
    line = jnp.where(jnp.bitwise_and(spot, 31) == 0, line, 0.0)
    terms[...] = jnp.broadcast_to(jnp.sum(line, axis=0, keepdims=True), (16, HD)).astype(BF16)


def transposed(a, b):
    return lax.dot_general(a, b, (((1,), (1,)), ((), ())), preferred_element_type=F32)


def thirds(value):
    high = value.astype(BF16).astype(F32)
    middle = (value - high).astype(BF16).astype(F32)
    return high, middle, value - high - middle


def attend_cached(cache_len, received, cache, terms, out):
    table = received[:, 64:72, :].reshape(128, HD)
    k = iota((128, 1), 0) % 8
    second = k >= 4
    second16 = second[0:16]
    scores = []
    for h in range(KVH):
        rows = table[16 * h : 16 * (h + 1)]
        both = [transposed(rows, cache[r, :, HD * h : HD * (h + 1)]) for r in range(2)]
        scores.append(jnp.where(second16, both[1], both[0]))
    score = jnp.concatenate(scores, axis=0) * SCALE
    count = jnp.where(second, cache_len[0:1, 1:2], cache_len[0:1, 0:1])
    alive = iota((128, HD), 1) < count
    highest = jnp.max(jnp.where(alive, score, LOWEST), axis=1, keepdims=True)
    exponent = jnp.where(alive, jnp.exp(score - highest), 0.0)
    total = jnp.sum(exponent, axis=1, keepdims=True)
    weight = (exponent / total).astype(BF16)
    values = []
    for h in range(KVH):
        rows = weight[16 * h : 16 * (h + 1)]
        at = HD * (KVH + h)
        both = [
            jnp.dot(rows, cache[r, :, at : at + HD], preferred_element_type=F32)
            for r in range(2)
        ]
        values.append(jnp.where(second16, both[1], both[0]))
    high, middle, low = thirds(highest + jnp.log(total))
    spot = iota((128, HD), 1) - k
    line = jnp.where(
        spot == 0, high, jnp.where(spot == 8, middle, jnp.where(spot == 16, low, 0.0))
    )
    line = jnp.sum(line.reshape(16, 8, HD), axis=1, keepdims=True)
    slot = iota((16, 8, HD), 1)
    rest = jnp.where(slot == 0, terms[0:1, :].astype(F32).reshape(1, 1, HD), line)
    result = jnp.concatenate(values, axis=0).reshape(16, 8, HD)
    out[...] = jnp.concatenate([result, rest], axis=1).astype(BF16)


def attend_prompts(parts, queries, lengths, owners, result, stats):
    prompts = prompts_of(
        lengths[...], owners[...], lax.axis_index("c8"), lax.axis_index("x")
    )
    request = iota((128, 1), 0) % 32
    landed, start, length = landing((request % 2) * 16 + request // 2, prompts)
    even = lax.axis_index("zl") == 0
    mine = jnp.concatenate([parts[x, 0:64] for x in range(4)], axis=0)
    other = jnp.concatenate([parts[x, 64:128] for x in range(4)], axis=0)
    keys = jnp.where(even, mine, other)
    values = jnp.where(even, other, mine)
    query = jnp.concatenate([queries[:, HD * i : HD * (i + 1)] for i in range(4)], axis=0)
    score = transposed(query, keys) * SCALE
    position = iota((128, 256), 1).astype(F32)
    alive = (position >= start) & (position < start + length)
    highest = jnp.max(jnp.where(alive, score, LOWEST), axis=1, keepdims=True)
    exponent = jnp.where(alive, jnp.exp(score - highest), 0.0)
    result[...] = jnp.dot(exponent.astype(BF16), values, preferred_element_type=F32)
    total = jnp.sum(exponent, axis=1, keepdims=True)
    lane = iota((128, HD), 1)
    stats[...] = jnp.where(lane == 0, highest, jnp.where(lane == 1, total, landed))


def finish(masked, received, queries, first, second, result, stats, logprob, attended, values, rows, sems):
    lines = received[:, 8, :].astype(F32)
    take = lambda k: lines[:, 32 * k : 32 * (k + 1)]
    peak, total = take(0), take(1) + take(2) + take(3)
    highest = jnp.max(peak, axis=0, keepdims=True)
    total = jnp.sum(total * jnp.exp(peak - highest), axis=0, keepdims=True)
    normalizer = highest + jnp.log(total)
    row, lane = iota((32, 32), 0), iota((32, 32), 1)
    normalizer = jnp.sum(jnp.where(row == lane, normalizer, 0.0), axis=1, keepdims=True)
    row = iota((128, 1), 0)
    head, request = row // 32, row % 32
    query = jnp.concatenate([queries[:, HD * i : HD * (i + 1)] for i in range(4)], axis=0)
    table = received[...].reshape(256, HD)
    place = (request % 2) * 4 + head
    slot = (request // 2) * 16
    picked = pick(jnp.concatenate([slot + place, slot + 9], axis=0), table)
    spot = iota((128, HD), 1) - place
    cached_top = jnp.where((spot == 0) | (spot == 8) | (spot == 16), picked[128:256], 0.0)
    cached_top = jnp.sum(cached_top, axis=1, keepdims=True)
    even = lax.axis_index("zl") == 0
    own_key = jnp.where(even, first[...], second[...]).astype(F32)
    own_value = jnp.where(even, second[...], first[...]).astype(F32)
    own_key = jnp.concatenate([own_key] * 4, axis=0)
    own_value = jnp.concatenate([own_value] * 4, axis=0)
    own = jnp.sum(query.astype(F32) * own_key, axis=1, keepdims=True) * SCALE
    landed = stats[:, 2:3] > 0.5
    top = jnp.where(landed, stats[:, 0:1], cached_top)
    total = jnp.where(landed, stats[:, 1:2], 1.0)
    live = jnp.where(landed, result[...], picked[0:128])
    highest = jnp.maximum(top, own)
    share, own_share = jnp.exp(top - highest), jnp.exp(own - highest)
    scale = 1.0 / (total * share + own_share)
    merged = ((live * share + own_value * own_share) * scale).astype(BF16)
    for i in range(4):
        rows[:, HD * i : HD * (i + 1)] = merged[32 * i : 32 * (i + 1)]
    copies = [pltpu.make_async_copy(rows, attended, sems.at[4])]
    copies[0].start()
    for b in range(4):
        at = slice(BLK * b, BLK * (b + 1))
        section = masked[:, at].astype(F32)
        values[:, at] = jnp.where(section == -jnp.inf, 0.0, section - normalizer)
        piece = pl.ds(BLK * b, BLK)
        copies.append(
            pltpu.make_async_copy(values.at[:, piece], logprob.at[:, piece], sems.at[b])
        )
        copies[-1].start()
    for copy in copies:
        copy.wait()


def exchanged(slots, axis):
    return lax.all_to_all(slots, axis, 0, 0, tiled=True)


def per_device(
    hidden,
    w_kv,
    prompt_lengths,
    owner_step,
    cache,
    cache_len,
    queries,
    fresh,
    logits,
    states,
    masks,
):
    vmem = pl.BlockSpec(memory_space=pltpu.VMEM)
    hbm = pl.BlockSpec(memory_space=pltpu.HBM)
    sent = jax.ShapeDtypeStruct
    kept = pltpu.VMEM
    held = lambda *values: [
        pltpu.with_memory_space_constraint(value, pltpu.VMEM) for value in values
    ]
    tokens, wide = hidden.shape[0] // 4, hidden.shape[1]
    shares = list(kernel(
        cut,
        out_shape=[kept((tokens, wide), BF16)] * 4,
        in_specs=[hbm],
        out_specs=[vmem] * 4,
        scratch_shapes=[pltpu.SemaphoreType.DMA((4,))],
        name="cut",
    )(pltpu.with_memory_space_constraint(hidden, pltpu.HBM)))
    for k in (1, 3, 2):
        shares[k] = lax.ppermute(shares[k], "x", [(0, k)])
    asked = kernel(
        pack,
        out_shape=kept((16, 8, HD), BF16),
        in_specs=[vmem],
        out_specs=vmem,
        name="pack",
        cost_estimate=pl.CostEstimate(
            flops=2000000000, bytes_accessed=1000, transcendentals=0
        ),
    )(*held(queries))
    projected = kernel(
        project,
        out_shape=pltpu.HBM((16, 72, HD), BF16),
        in_specs=[vmem] * 6,
        out_specs=hbm,
        scratch_shapes=[pltpu.VMEM((16, 72, HD), BF16), pltpu.SemaphoreType.DMA((4,))],
        name="project",
    )(*held(*shares, asked, w_kv))
    pieces = exchanged(projected, TP)
    keys_first = [(b, 2 * b) if b < KVH else (b, 2 * (b - KVH) + 1) for b in range(16)]
    values_first = [(b, d + 1 - 2 * (d % 2)) for b, d in keys_first]
    renewed = [lax.ppermute(fresh, TP, route) for route in (keys_first, values_first)]
    masked, terms = kernel(
        grammar,
        out_shape=[kept(logits.shape, BF16), kept((16, HD), BF16)],
        in_specs=[vmem] * 3,
        out_specs=[vmem] * 2,
        name="grammar",
    )(*held(logits, states.reshape(1, -1), masks))
    block = kernel(
        reduce_blocks,
        out_shape=kept((tokens, HD), BF16),
        in_specs=[vmem],
        out_specs=vmem,
        name="reduce",
    )(*held(pieces))
    other = lax.ppermute(block, "zl", [(0, 1), (1, 0)])
    answers = kernel(
        attend_cached,
        out_shape=sent((16, 16, HD), BF16),
        in_specs=[vmem] * 4,
        name="cached",
    )(*held(cache_len.reshape(1, 2), pieces, cache, terms))
    answers = exchanged(answers, TP)
    both = jnp.concatenate([block, other], axis=0)
    around = lax.all_gather(both, "x")
    result, stats = kernel(
        attend_prompts,
        out_shape=[kept((128, HD), F32), kept((128, HD), F32)],
        in_specs=[vmem] * 4,
        out_specs=[vmem] * 2,
        name="prompts",
    )(*held(around, queries, prompt_lengths, owner_step))
    logprob, attended = kernel(
        finish,
        out_shape=[pltpu.HBM(logits.shape, F32), pltpu.HBM(queries.shape, BF16)],
        in_specs=[vmem] * 7,
        out_specs=[hbm, hbm],
        scratch_shapes=[
            pltpu.VMEM(logits.shape, F32),
            pltpu.VMEM(queries.shape, BF16),
            pltpu.SemaphoreType.DMA((5,)),
        ],
        name="finish",
    )(*held(masked, answers, queries, *renewed, result, stats))
    return attended, logprob


def solution(mesh):
    groups, columns = mesh.shape["group"], mesh.shape["tp"]
    finer = Mesh(
        mesh.devices.reshape(4, groups // 4, columns // 2, 2), ("x", "c8", "zh", "zl")
    )
    group = ("x", "c8")
    in_specs = (
        P(group, TP),
        P(TP, None),
        P(),
        P(),
        P(group + TP, None, None),
        P(group + TP),
        P(group, TP),
        P(group, TP),
        P(group, TP),
        P(group),
        P(None, TP),
    )
    return jax.shard_map(
        per_device,
        mesh=finer,
        in_specs=in_specs,
        out_specs=(P(group, TP), P(group, TP)),
        check_vma=False,
    )
```
